8 devices in a mesh: data: 1 (over z), col: 2 (over y), row: 4 (over x, core).
Axes of the slice: x: 2, y: 2, z: 1, core: 2. Of those that a mesh axis runs over, the one named last changes fastest.
Arguments:
- x_seq: bfloat16 [64, 8, 2560], P(None, 'data', 'row')
- h_init: float32 [2, 8, 2560], P(None, 'data', 'row')
- wx_l1: bfloat16 [2560, 3, 2560], P('row', None, 'col')
- whru_l1: bfloat16 [2560, 2, 2560], P('row', None, 'col')
- whn_l1: bfloat16 [2560, 2560], P('row', 'col')
- bias_l1: float32 [3, 2560], P(None, 'col')
- wx_l2: bfloat16 [2560, 3, 2560], P('row', None, 'col')
- whru_l2: bfloat16 [2560, 2, 2560], P('row', None, 'col')
- whn_l2: bfloat16 [2560, 2560], P('row', 'col')
- bias_l2: float32 [3, 2560], P(None, 'col')
Outputs:
- output 1: bfloat16 [64, 8, 2560], P(None, 'data', ('col', 'row'))
- output 2: float32 [2, 8, 2560], P(None, 'data', ('col', 'row'))
All inputs are finite; a program needn't handle non-finite values.
Results may differ from the reference program's by a relative error of at most 0.00269291.
Values are sent between devices in bfloat16 or wider.
A program may use at most 1 GiB of HBM per device.

```python
import jax
import jax.numpy as jnp
from jax import lax

SEQ_LEN = 64
BATCH_GROUP = 8
HIDDEN = 2560


def setup_inputs(seed: int = 0, part: int = 0) -> dict:
    part_key = jax.random.fold_in(jax.random.key(seed), part)
    seq_key, state_key = jax.random.split(part_key, 2)
    weight_keys = jax.random.split(jax.random.key(seed + 1), 8)
    w_scale = HIDDEN ** -0.5
    gate_shift = jnp.array([0.0, 1.5, 0.0], jnp.float32)[:, None]

    def draw_weight(key, shape):
        return (w_scale * jax.random.normal(key, shape, jnp.float32)).astype(jnp.bfloat16)

    def draw_bias(key):
        return 0.5 * jax.random.normal(key, (3, HIDDEN), jnp.float32) + gate_shift

    x_seq = jax.random.normal(seq_key, (SEQ_LEN, BATCH_GROUP, HIDDEN), jnp.float32).astype(jnp.bfloat16)
    h_init = 0.8 * jnp.tanh(jax.random.normal(state_key, (2, BATCH_GROUP, HIDDEN), jnp.float32))
    return {
        "x_seq": x_seq,
        "h_init": h_init,
        "wx_l1": draw_weight(weight_keys[0], (HIDDEN, 3, HIDDEN)),
        "whru_l1": draw_weight(weight_keys[1], (HIDDEN, 2, HIDDEN)),
        "whn_l1": draw_weight(weight_keys[2], (HIDDEN, HIDDEN)),
        "bias_l1": draw_bias(weight_keys[3]),
        "wx_l2": draw_weight(weight_keys[4], (HIDDEN, 3, HIDDEN)),
        "whru_l2": draw_weight(weight_keys[5], (HIDDEN, 2, HIDDEN)),
        "whn_l2": draw_weight(weight_keys[6], (HIDDEN, HIDDEN)),
        "bias_l2": draw_bias(weight_keys[7]),
    }


def gru_layer(in_seq, w_x, w_hru, w_hn, gate_bias, h_start):
    batch_rows = in_seq.shape[1]
    wx_flat = w_x.reshape(HIDDEN, 3 * HIDDEN)
    whru_flat = w_hru.reshape(HIDDEN, 2 * HIDDEN)

    def gru_step(h_prev, step_in):
        in_proj = jnp.dot(step_in, wx_flat, preferred_element_type=jnp.float32).reshape(batch_rows, 3, HIDDEN) + gate_bias
        rec_ru = jnp.dot(h_prev.astype(jnp.bfloat16), whru_flat, preferred_element_type=jnp.float32).reshape(batch_rows, 2, HIDDEN)
        reset_gate = jax.nn.sigmoid(in_proj[:, 0] + rec_ru[:, 0])
        update_gate = jax.nn.sigmoid(in_proj[:, 1] + rec_ru[:, 1])
        gated_h = (reset_gate * h_prev).astype(jnp.bfloat16)
        candidate = jnp.tanh(in_proj[:, 2] + jnp.dot(gated_h, w_hn, preferred_element_type=jnp.float32))
        h_next = (1.0 - update_gate) * candidate + update_gate * h_prev
        return h_next, h_next.astype(jnp.bfloat16)

    return lax.scan(gru_step, h_start, in_seq)


def reference(x_seq, h_init, wx_l1, whru_l1, whn_l1, bias_l1, wx_l2, whru_l2, whn_l2, bias_l2):
    h1_last, h1_seq = gru_layer(x_seq, wx_l1, whru_l1, whn_l1, bias_l1, h_init[0])
    h2_last, h2_seq = gru_layer(h1_seq, wx_l2, whru_l2, whn_l2, bias_l2, h_init[1])
    return h2_seq, jnp.stack([h1_last, h2_last])
```

```python
import functools

import jax
import jax.numpy as jnp
from jax import lax
from jax.experimental import pallas as pl
from jax.experimental.pallas import tpu as pltpu
from jax.sharding import PartitionSpec as P

MESH = pl.DeviceIdType.MESH
F32 = jnp.float32
BF16 = jnp.bfloat16

STEPS = 64
BATCH = 8
HALF = 1280
ROWS = 640
PART = 640
OWN = 320
CHUNK = 8
CHUNKS = STEPS // CHUNK
RING = 4


def gru_kernel(w_in, wx_in, p_in, h0, bias, seq_out, fin_out,
               w, pbuf, hid, rhb, state, outbuf, oscr, finsrc, finbuf,
               w_send, w_recv, wx_send, wx_recv, p_send, p_recv, h_send, h_recv,
               n_send, r_send, r_recv, o_send, o_recv, f_send, f_recv):
    row = lax.axis_index("row")
    col = lax.axis_index("col")
    chip = row // 2
    core = row % 2
    other = 1 - core
    hub = chip == col
    layer = chip

    def device(r, c):
        return {"row": r, "col": c}

    def remote(src, dst, send, recv, r, c):
        return pltpu.make_async_remote_copy(
            src_ref=src, dst_ref=dst, send_sem=send, recv_sem=recv,
            device_id=device(r, c), device_id_type=MESH)

    def arrived(ref, sem):
        pltpu.make_async_copy(ref, ref, sem).wait()

    def p_copy(k):
        at = pl.ds(k * CHUNK, CHUNK)
        return p_in.at[at], pbuf.at[chip, core, at], p_send.at[k], p_recv.at[k, chip, core], col, 0

    slot = jnp.where(hub, 0, 1)
    my_rows = pl.ds(core * ROWS, ROWS)

    def w_copy(l):
        return w_in.at[l], w.at[slot, my_rows], w_send.at[l], w_recv.at[slot, core], 2 * l + col, l

    def wx_copy(half):
        return (wx_in.at[half], w.at[chip, my_rows, pl.ds(0, 3 * PART)], wx_send.at[half],
                wx_recv.at[row], 2 * (1 - col) + half, col)

    def start(spec):
        src, dst, send, recv, r, c = spec
        here = (r == row) & (c == col)

        @pl.when(here)
        def _():
            pltpu.make_async_copy(src, dst, recv).start()

        @pl.when(jnp.logical_not(here))
        def _():
            remote(src, dst, send, recv, r, c).start()

    def finish(spec):
        src, dst, send, recv, r, c = spec
        here = (r == row) & (c == col)

        @pl.when(jnp.logical_not(here))
        def _():
            remote(src, dst, send, recv, r, c).wait_send()

    start(p_copy(0))
    start(w_copy(0))
    start(w_copy(1))
    for half in range(2):
        start(wx_copy(half))
    for k in range(1, CHUNKS):
        start(p_copy(k))

    @pl.when(hub)
    def _():
        first = layer == 0
        for b in range(2):
            hid[0, b] = h0[layer, :, b * HALF:(b + 1) * HALF].astype(BF16)
        state[...] = h0[layer, :, pl.ds(pl.multiple_of(core * HALF, HALF), HALF)]

        @pl.when(jnp.logical_not(first))
        def _():
            def clear(t, carry):
                for b in range(2):
                    pbuf[1, b, t] = jnp.zeros((BATCH, 3 * PART), F32)
                return carry
            lax.fori_loop(0, STEPS, clear, 0)

        for s in range(2):
            for b in range(2):
                arrived(w.at[s, pl.ds(b * ROWS, ROWS)], w_recv.at[s, b])

        def partner(t):
            return remote(hid.at[t, core], hid.at[t, core], n_send.at[t % RING], h_recv.at[t, core],
                          2 * chip + other, col)

        def helper(t, y, b):
            return remote(hid.at[t, core], hid.at[t, core], h_send.at[t % RING, y, b], h_recv.at[t, core],
                          2 * (1 - y) + b, y)

        def piece(i, k):
            at = pl.ds(k * CHUNK, CHUNK)
            return remote(outbuf.at[i, at], oscr.at[at], o_send.at[i, k], o_recv.at[k], i, core)

        def mine(i):
            return (row == i) & (col == core)

        def gate(t, g):
            cols = pl.ds(g * PART, PART)
            return jnp.concatenate(
                [pbuf[0, b, t, :, cols] + pbuf[1, b, t, :, cols] for b in range(2)], axis=1)

        def tick(t, carry):
            @pl.when(first & (t % CHUNK == 0))
            def _():
                k = t // CHUNK
                at = pl.ds(k * CHUNK, CHUNK)
                for a in range(2):
                    for b in range(2):
                        arrived(pbuf.at[a, b, at], p_recv.at[k, a, b])

            @pl.when(jnp.logical_not(first))
            def _():
                for b in range(2):
                    arrived(pbuf.at[0, b, t], p_recv.at[t, 0, b])

            ru_own = jnp.dot(hid[t, core], w[0, :, 0:2 * HALF], preferred_element_type=F32)

            @pl.when(t > 0)
            def _():
                partner(t).wait_send()
                arrived(hid.at[t, other], h_recv.at[t, other])

            r_sum = ru_own[:, 0:HALF] + jnp.dot(hid[t, other], w[1, :, 0:HALF], preferred_element_type=F32)
            reset = jax.nn.sigmoid(gate(t, 0) + r_sum)
            q = t % 2
            rhb[q, core] = (reset * state[...]).astype(BF16)
            swap = remote(rhb.at[q, core], rhb.at[q, core], r_send.at[q], r_recv.at[q], 2 * chip + other, col)
            swap.start()
            u_sum = ru_own[:, HALF:] + jnp.dot(hid[t, other], w[1, :, HALF:2 * HALF], preferred_element_type=F32)
            update = jax.nn.sigmoid(gate(t, 1) + u_sum)
            n_sum = gate(t, 2) + jnp.dot(rhb[q, core], w[0, :, 2 * HALF:], preferred_element_type=F32)
            swap.wait_send()
            arrived(rhb.at[q, other], r_recv.at[q])
            n_sum = n_sum + jnp.dot(rhb[q, other], w[1, :, 2 * HALF:], preferred_element_type=F32)
            cand = jnp.tanh(n_sum)
            h_next = (1.0 - update) * cand + update * state[...]
            state[...] = h_next
            h_bf = h_next.astype(BF16)
            hid[t + 1, core] = h_bf

            @pl.when(t < STEPS - 1)
            def _():
                partner(t + 1).start()

            @pl.when(first)
            def _():
                for y in range(2):
                    for b in range(2):
                        @pl.when(t >= RING)
                        def _():
                            helper(t + 1 - RING, y, b).wait_send()
                        helper(t + 1, y, b).start()

            @pl.when(jnp.logical_not(first))
            def _():
                for i in range(4):
                    outbuf[i, t] = h_bf[:, i * OWN:(i + 1) * OWN]

                @pl.when(t % CHUNK == CHUNK - 1)
                def _():
                    for i in range(4):
                        @pl.when(jnp.logical_not(mine(i)))
                        def _():
                            piece(i, t // CHUNK).start()
            return carry

        lax.fori_loop(0, STEPS, tick, 0)

        last = state[...]
        for i in range(4):
            finsrc[i] = last[:, i * OWN:(i + 1) * OWN]

        def fin_copy(i):
            return remote(finsrc.at[i], finbuf.at[layer], f_send.at[i], f_recv.at[layer], i, core)

        for i in range(4):
            @pl.when(mine(i))
            def _():
                finbuf[layer] = finsrc[i]

                @pl.when(jnp.logical_not(first))
                def _():
                    def take(t, carry):
                        oscr[t] = outbuf[i, t]
                        return carry
                    lax.fori_loop(0, STEPS, take, 0)

            @pl.when(jnp.logical_not(mine(i)))
            def _():
                fin_copy(i).start()

        for i in range(4):
            @pl.when(jnp.logical_not(mine(i)))
            def _():
                fin_copy(i).wait_send()

                @pl.when(jnp.logical_not(first))
                def _():
                    for k in range(CHUNKS):
                        piece(i, k).wait_send()

        @pl.when(first)
        def _():
            for t in range(STEPS + 1 - RING, STEPS + 1):
                for y in range(2):
                    for b in range(2):
                        helper(t, y, b).wait_send()

    @pl.when(jnp.logical_not(hub))
    def _():
        for i in range(4):
            arrived(w.at[i // 2, pl.ds((i % 2) * ROWS, ROWS), pl.ds(0, 3 * PART)], wx_recv.at[i])

        def project(t):
            return remote(pbuf.at[0, core, t], pbuf.at[0, core, t], h_send.at[t % RING, 0, 0],
                          p_recv.at[t, 0, core], 2 + col, 1)

        def tick(t, carry):
            for b in range(2):
                arrived(hid.at[t + 1, b], h_recv.at[t + 1, b])
            total = jnp.dot(hid[t + 1, 0], w[0, :, 0:3 * PART], preferred_element_type=F32)
            total = total + jnp.dot(hid[t + 1, 1], w[1, :, 0:3 * PART], preferred_element_type=F32)
            pbuf[0, core, t] = total + bias[...]

            @pl.when(t >= RING)
            def _():
                project(t - RING).wait_send()
            project(t).start()
            return carry

        lax.fori_loop(0, STEPS, tick, 0)
        for t in range(STEPS - RING, STEPS):
            project(t).wait_send()

    for l in range(2):
        finish(w_copy(l))
        finish(wx_copy(l))
    for k in range(CHUNKS):
        finish(p_copy(k))
    for l in range(2):
        @pl.when(jnp.logical_not((row == 2 * l + col) & (col == l)))
        def _():
            arrived(finbuf.at[l], f_recv.at[l])

    @pl.when(jnp.logical_not((row == 2 + col) & (col == 1)))
    def _():
        for k in range(CHUNKS):
            at = pl.ds(k * CHUNK, CHUNK)
            arrived(oscr.at[at], o_recv.at[k])

    def emit(t, carry):
        seq_out[t] = oscr[t]
        return carry
    lax.fori_loop(0, STEPS, emit, 0)
    fin_out[...] = finbuf[...]


def gru_call(w_in, wx_in, p_in, h0, bias):
    dma = pltpu.SemaphoreType.DMA
    any_spec = pl.BlockSpec(memory_space=pl.ANY)
    vmem_spec = pl.BlockSpec(memory_space=pltpu.VMEM)
    return pl.pallas_call(
        gru_kernel,
        out_shape=(jax.ShapeDtypeStruct((STEPS, BATCH, OWN), BF16), jax.ShapeDtypeStruct((2, BATCH, OWN), F32)),
        in_specs=[any_spec, any_spec, any_spec, vmem_spec, vmem_spec],
        out_specs=(vmem_spec, vmem_spec),
        scratch_shapes=[
            pltpu.VMEM((2, HALF, 3 * HALF), BF16),
            pltpu.VMEM((2, 2, STEPS, BATCH, 3 * PART), F32),
            pltpu.VMEM((STEPS + 1, 2, BATCH, HALF), BF16),
            pltpu.VMEM((2, 2, BATCH, HALF), BF16),
            pltpu.VMEM((BATCH, HALF), F32),
            pltpu.VMEM((4, STEPS, BATCH, OWN), BF16),
            pltpu.VMEM((STEPS, BATCH, OWN), BF16),
            pltpu.VMEM((4, BATCH, OWN), F32),
            pltpu.VMEM((2, BATCH, OWN), F32),
            dma((2,)), dma((2, 2)),
            dma((2,)), dma((4,)),
            dma((CHUNKS,)), dma((STEPS, 2, 2)),
            dma((RING, 2, 2)), dma((STEPS + 1, 2)),
            dma((RING,)), dma((2,)), dma((2,)),
            dma((4, CHUNKS)), dma((CHUNKS,)),
            dma((4,)), dma((2,)),
        ],
        compiler_params=pltpu.CompilerParams(has_side_effects=True, vmem_limit_bytes=62 * 2**20),
        name="gru",
    )(w_in, wx_in, p_in, h0, bias)


def solution(mesh):
    seq_spec = P(None, "data", "row")
    out_spec = P(None, "data", ("col", "row"))
    wide_spec = P("row", None, "col")
    square_spec = P("row", "col")
    bias_spec = P(None, "col")
    swap = [(0, 1), (1, 0), (2, 3), (3, 2)]

    def halves(w):
        return w.reshape(ROWS, 3, 2, PART).transpose(2, 0, 1, 3).reshape(2, ROWS, 3 * PART)

    def device_body(x_rows, h_rows, wx_l1, whru_l1, whn_l1, bias_l1, wx_l2, whru_l2, whn_l2, bias_l2):
        row = lax.axis_index("row")
        core = row % 2
        chip = row // 2

        def bias_half(b):
            return lax.dynamic_index_in_dim(b.reshape(3, 2, PART), core, 1, keepdims=False).reshape(1, 3 * PART)

        wx1 = halves(wx_l1)
        own = lax.dynamic_index_in_dim(wx1, core, 0, keepdims=False)
        theirs = lax.ppermute(lax.dynamic_index_in_dim(wx1, 1 - core, 0, keepdims=False), "row", swap)
        x_own = x_rows.reshape(STEPS * BATCH, ROWS)
        x_theirs = lax.ppermute(x_own, "row", swap)
        p1 = jnp.dot(x_own, own, preferred_element_type=F32) + jnp.dot(x_theirs, theirs, preferred_element_type=F32)
        p1 = p1 + jnp.where(chip == 0, bias_half(bias_l1), 0.0)
        p1 = p1.reshape(STEPS, BATCH, 3 * PART)

        h0 = lax.all_gather(h_rows, "row", axis=2, tiled=True)
        w_rec = jnp.stack([
            jnp.concatenate([whru_l1.reshape(ROWS, 2 * HALF), whn_l1], axis=1),
            jnp.concatenate([whru_l2.reshape(ROWS, 2 * HALF), whn_l2], axis=1)])
        return gru_call(w_rec, halves(wx_l2), p1, h0, bias_half(bias_l2))

    return jax.shard_map(
        device_body,
        mesh=mesh,
        in_specs=(seq_spec, seq_spec, wide_spec, wide_spec, square_spec, bias_spec, wide_spec, wide_spec, square_spec, bias_spec),
        out_specs=(out_spec, out_spec),
        check_vma=False,
    )
```

```python
import functools

import jax
import jax.numpy as jnp
from jax import lax
from jax.experimental import pallas as pl
from jax.experimental.pallas import tpu as pltpu
from jax.sharding import PartitionSpec as P

MESH = pl.DeviceIdType.MESH
F32 = jnp.float32
BF16 = jnp.bfloat16

STEPS = 64
BATCH = 8
HALF = 1280
ROWS = 640
PART = 640
OWN = 320
CHUNK = 8
CHUNKS = STEPS // CHUNK
RING = 4


def gru_kernel(x_in, wx1_in, wx2_in, ru1_in, ru2_in, n1_in, n2_in, h_in, bias1, bias2, seq_out, fin_out,
               w, pbuf, psrc, xs, wx1, h0, hid, rhb, state, outbuf, oscr, finsrc, finbuf,
               x_send, x_recv, v_send, v_recv, z_send, z_recv, s_send, s_recv, t_send,
               w_send, w_recv, wx_send, wx_recv, p_send, p_recv, h_send, h_recv,
               n_send, r_send, r_recv, o_send, o_recv, f_send, f_recv):
    row = lax.axis_index("row")
    col = lax.axis_index("col")
    chip = row // 2
    core = row % 2
    other = 1 - core
    hub = chip == col
    layer = chip

    def device(r, c):
        return {"row": r, "col": c}

    def remote(src, dst, send, recv, r, c):
        return pltpu.make_async_remote_copy(
            src_ref=src, dst_ref=dst, send_sem=send, recv_sem=recv,
            device_id=device(r, c), device_id_type=MESH)

    def arrived(ref, sem):
        pltpu.make_async_copy(ref, ref, sem).wait()

    def start(spec):
        src, dst, send, recv, r, c = spec
        here = (r == row) & (c == col)

        @pl.when(here)
        def _():
            pltpu.make_async_copy(src, dst, recv).start()

        @pl.when(jnp.logical_not(here))
        def _():
            remote(src, dst, send, recv, r, c).start()

    def finish(spec):
        src, dst, send, recv, r, c = spec
        here = (r == row) & (c == col)

        @pl.when(jnp.logical_not(here))
        def _():
            remote(src, dst, send, recv, r, c).wait_send()

    slot = jnp.where(hub, 0, 1)
    my_rows = pl.ds(core * ROWS, ROWS)
    my_cols = pl.ds(pl.multiple_of(core * ROWS, ROWS), ROWS)

    def gate_cols(g):
        return pl.ds(g * HALF, HALF)

    def weight(l, g):
        return (n1_in, n2_in)[l] if g == 2 else (ru1_in, ru2_in)[l].at[g]

    def x_copy(to):
        return x_in, xs.at[:, my_cols], x_send.at[0], x_recv.at[core], 2 * chip + to, col

    def wx1_copy(to, g):
        half = pl.ds(pl.multiple_of(to * PART, PART), PART)
        return (wx1_in.at[g, :, half], wx1.at[my_rows, pl.ds(g * PART, PART)], v_send.at[g], v_recv.at[core, g],
                2 * chip + to, col)

    def h0_copy(to):
        return h_in.at[col], h0.at[row], z_send.at[to], z_recv.at[row], 2 * col + to, col

    def w_copy(l, g):
        return (weight(l, g), w.at[slot, my_rows, gate_cols(g)], w_send.at[l, g], w_recv.at[slot, core, g, 0],
                2 * l + col, l)

    def stage_rows(g):
        return pl.ds(g * (ROWS // 2), ROWS // 2)

    stage_cols = pl.ds(3 * PART, HALF)

    def stage_copy(l, h, g):
        src = weight(1 - l, g).at[pl.ds(h * (ROWS // 2), ROWS // 2)]
        r, c = (2 * (1 - l) + core, l) if h == 0 else (2 * l + core, 1 - l)
        return src, w.at[l, stage_rows(g), stage_cols], s_send.at[h, g], s_recv.at[l, g], r, c

    def forward_copy(l, g):
        h = jnp.where(col == l, 0, 1)
        rows = pl.ds(core * ROWS + h * (ROWS // 2), ROWS // 2)
        return (w.at[l, stage_rows(g), stage_cols], w.at[0, rows, gate_cols(g)], t_send.at[l, g],
                w_recv.at[0, core, g, h], 2 * (1 - l) + l, 1 - l)

    def wx_copy(half, g):
        return (wx2_in.at[g, :, pl.ds(half * PART, PART)], w.at[chip, my_rows, pl.ds(g * PART, PART)],
                wx_send.at[half, g], wx_recv.at[row, g], 2 * (1 - col) + half, col)

    def p_copy(k):
        at = pl.ds(k * CHUNK, CHUNK)
        return psrc.at[at], pbuf.at[chip, core, at], p_send.at[k], p_recv.at[k, chip, core], col, 0

    for to in (core, other):
        start(x_copy(to))
        for g in range(3):
            start(wx1_copy(to, g))
    for to in range(2):
        start(h0_copy(to))
    for l in range(2):
        @pl.when(hub & (chip == l))
        def _():
            for g in range(3):
                for h in range(2):
                    start(stage_copy(l, h, g))
            for g in range(3):
                start(w_copy(l, g))

    @pl.when(jnp.logical_not(hub))
    def _():
        for g in range(2):
            for l in range(2):
                start(w_copy(l, g))

    for b in range(2):
        arrived(xs.at[:, pl.ds(b * ROWS, ROWS)], x_recv.at[b])
        for g in range(3):
            arrived(wx1.at[pl.ds(b * ROWS, ROWS), pl.ds(g * PART, PART)], v_recv.at[b, g])

    def bias_of(ref, g):
        return ref[g:g + 1, my_cols]

    def project_x(k, carry):
        lines = xs[pl.ds(k * CHUNK * BATCH, CHUNK * BATCH), :]
        for g in range(3):
            total = jnp.dot(lines, wx1[:, g * PART:(g + 1) * PART], preferred_element_type=F32)
            total = total + jnp.where(chip == 0, bias_of(bias1, g), 0.0)
            psrc[pl.ds(k * CHUNK, CHUNK), :, g * PART:(g + 1) * PART] = total.reshape(CHUNK, BATCH, PART)
        return carry

    lax.fori_loop(0, CHUNKS, project_x, 0)
    start(p_copy(0))

    for l in range(2):
        @pl.when(hub & (chip == l))
        def _():
            for g in range(3):
                for h in range(2):
                    finish(stage_copy(l, h, g))
            for g in range(3):
                for half in range(2):
                    start(wx_copy(half, g))
            if l == 1:
                for g in range(3):
                    for half in range(2):
                        finish(wx_copy(half, g))

    @pl.when(jnp.logical_not(hub))
    def _():
        for l in range(2):
            start(w_copy(l, 2))
        for g in range(3):
            for half in range(2):
                start(wx_copy(half, g))
        for g in range(3):
            for l in range(2):
                arrived(w.at[l, stage_rows(g), stage_cols], s_recv.at[l, g])
                start(forward_copy(l, g))
        for g in range(3):
            for l in range(2):
                finish(w_copy(l, g))
                finish(forward_copy(l, g))

    for k in range(1, CHUNKS):
        start(p_copy(k))

    @pl.when(hub)
    def _():
        first = layer == 0
        for i in range(4):
            arrived(h0.at[i], z_recv.at[i])
        for b in range(2):
            hid[0, b] = jnp.concatenate([h0[2 * b], h0[2 * b + 1]], axis=1).astype(BF16)
        state[...] = jnp.concatenate([h0[2 * core], h0[2 * core + 1]], axis=1)

        @pl.when(jnp.logical_not(first))
        def _():
            def clear(t, carry):
                for b in range(2):
                    pbuf[1, b, t] = jnp.zeros((BATCH, 3 * PART), F32)
                return carry
            lax.fori_loop(0, STEPS, clear, 0)

        def weights_in(s, b, g, h, rows):
            at = pl.ds(b * ROWS + h * (ROWS // 2), rows)
            arrived(w.at[s, at, gate_cols(g)], w_recv.at[s, b, g, h])

        for g in range(3):
            for b in range(2):
                weights_in(1, b, g, 0, ROWS)

                @pl.when(core == chip)
                def _():
                    weights_in(0, b, g, 0, ROWS)

                @pl.when(core != chip)
                def _():
                    for h in range(2):
                        weights_in(0, b, g, h, ROWS // 2)

        def partner(t):
            return remote(hid.at[t, core], hid.at[t, core], n_send.at[t % RING], h_recv.at[t, core],
                          2 * chip + other, col)

        def helper(t, y, b):
            return remote(hid.at[t, core], hid.at[t, core], h_send.at[t % RING, y, b], h_recv.at[t, core],
                          2 * (1 - y) + b, y)

        def piece(i, k):
            at = pl.ds(k * CHUNK, CHUNK)
            return remote(outbuf.at[i, at], oscr.at[at], o_send.at[i, k], o_recv.at[k], i, core)

        def mine(i):
            return (row == i) & (col == core)

        def gate(t, g):
            cols = pl.ds(g * PART, PART)
            return jnp.concatenate(
                [pbuf[0, b, t, :, cols] + pbuf[1, b, t, :, cols] for b in range(2)], axis=1)

        def tick(t, carry):
            @pl.when(first & (t % CHUNK == 0))
            def _():
                k = t // CHUNK
                at = pl.ds(k * CHUNK, CHUNK)
                for a in range(2):
                    for b in range(2):
                        arrived(pbuf.at[a, b, at], p_recv.at[k, a, b])

            @pl.when(jnp.logical_not(first))
            def _():
                for b in range(2):
                    arrived(pbuf.at[0, b, t], p_recv.at[t, 0, b])

            ru_own = jnp.dot(hid[t, core], w[0, :, 0:2 * HALF], preferred_element_type=F32)

            @pl.when(t > 0)
            def _():
                partner(t).wait_send()
                arrived(hid.at[t, other], h_recv.at[t, other])

            r_sum = ru_own[:, 0:HALF] + jnp.dot(hid[t, other], w[1, :, 0:HALF], preferred_element_type=F32)
            reset = jax.nn.sigmoid(gate(t, 0) + r_sum)
            q = t % 2
            rhb[q, core] = (reset * state[...]).astype(BF16)
            swap = remote(rhb.at[q, core], rhb.at[q, core], r_send.at[q], r_recv.at[q], 2 * chip + other, col)
            swap.start()
            u_sum = ru_own[:, HALF:] + jnp.dot(hid[t, other], w[1, :, HALF:2 * HALF], preferred_element_type=F32)
            update = jax.nn.sigmoid(gate(t, 1) + u_sum)
            n_sum = gate(t, 2) + jnp.dot(rhb[q, core], w[0, :, 2 * HALF:], preferred_element_type=F32)
            swap.wait_send()
            arrived(rhb.at[q, other], r_recv.at[q])
            n_sum = n_sum + jnp.dot(rhb[q, other], w[1, :, 2 * HALF:], preferred_element_type=F32)
            cand = jnp.tanh(n_sum)
            h_next = (1.0 - update) * cand + update * state[...]
            state[...] = h_next
            h_bf = h_next.astype(BF16)
            hid[t + 1, core] = h_bf

            @pl.when(t < STEPS - 1)
            def _():
                partner(t + 1).start()

            @pl.when(first)
            def _():
                for y in range(2):
                    for b in range(2):
                        @pl.when(t >= RING)
                        def _():
                            helper(t + 1 - RING, y, b).wait_send()
                        helper(t + 1, y, b).start()

            @pl.when(jnp.logical_not(first))
            def _():
                for i in range(4):
                    outbuf[i, t] = h_bf[:, i * OWN:(i + 1) * OWN]

                @pl.when(t % CHUNK == CHUNK - 1)
                def _():
                    for i in range(4):
                        @pl.when(jnp.logical_not(mine(i)))
                        def _():
                            piece(i, t // CHUNK).start()
            return carry

        lax.fori_loop(0, STEPS, tick, 0)

        last = state[...]
        for i in range(4):
            finsrc[i] = last[:, i * OWN:(i + 1) * OWN]

        def fin_copy(i):
            return remote(finsrc.at[i], finbuf.at[layer], f_send.at[i], f_recv.at[layer], i, core)

        for i in range(4):
            @pl.when(mine(i))
            def _():
                finbuf[layer] = finsrc[i]

                @pl.when(jnp.logical_not(first))
                def _():
                    def take(t, carry):
                        oscr[t] = outbuf[i, t]
                        return carry
                    lax.fori_loop(0, STEPS, take, 0)

            @pl.when(jnp.logical_not(mine(i)))
            def _():
                fin_copy(i).start()

        for i in range(4):
            @pl.when(jnp.logical_not(mine(i)))
            def _():
                fin_copy(i).wait_send()

                @pl.when(jnp.logical_not(first))
                def _():
                    for k in range(CHUNKS):
                        piece(i, k).wait_send()

        @pl.when(first)
        def _():
            for t in range(STEPS + 1 - RING, STEPS + 1):
                for y in range(2):
                    for b in range(2):
                        helper(t, y, b).wait_send()

    @pl.when(jnp.logical_not(hub))
    def _():
        for g in range(3):
            for i in range(4):
                arrived(w.at[i // 2, pl.ds((i % 2) * ROWS, ROWS), pl.ds(g * PART, PART)], wx_recv.at[i, g])

        def project(t):
            return remote(pbuf.at[0, core, t], pbuf.at[0, core, t], h_send.at[t % RING, 0, 0],
                          p_recv.at[t, 0, core], 2 + col, 1)

        def tick(t, carry):
            for b in range(2):
                arrived(hid.at[t + 1, b], h_recv.at[t + 1, b])
            total = jnp.dot(hid[t + 1, 0], w[0, :, 0:3 * PART], preferred_element_type=F32)
            total = total + jnp.dot(hid[t + 1, 1], w[1, :, 0:3 * PART], preferred_element_type=F32)
            shift = jnp.concatenate([bias_of(bias2, g) for g in range(3)], axis=1)
            pbuf[0, core, t] = total + shift

            @pl.when(t >= RING)
            def _():
                project(t - RING).wait_send()
            project(t).start()
            return carry

        lax.fori_loop(0, STEPS, tick, 0)
        for t in range(STEPS - RING, STEPS):
            project(t).wait_send()

    for l in range(2):
        @pl.when(hub & (chip == l))
        def _():
            for g in range(3):
                finish(w_copy(l, g))
                if l == 0:
                    for half in range(2):
                        finish(wx_copy(half, g))

    @pl.when(jnp.logical_not(hub))
    def _():
        for g in range(3):
            for half in range(2):
                finish(wx_copy(half, g))
    finish(x_copy(other))
    for g in range(3):
        finish(wx1_copy(other, g))
    for to in range(2):
        finish(h0_copy(to))
    for k in range(CHUNKS):
        finish(p_copy(k))
    for l in range(2):
        @pl.when(jnp.logical_not((row == 2 * l + col) & (col == l)))
        def _():
            arrived(finbuf.at[l], f_recv.at[l])

    @pl.when(jnp.logical_not((row == 2 + col) & (col == 1)))
    def _():
        for k in range(CHUNKS):
            at = pl.ds(k * CHUNK, CHUNK)
            arrived(oscr.at[at], o_recv.at[k])

    def emit(t, carry):
        seq_out[t] = oscr[t]
        return carry
    lax.fori_loop(0, STEPS, emit, 0)
    fin_out[...] = finbuf[...]


def gru_call(*operands):
    dma = pltpu.SemaphoreType.DMA
    any_spec = pl.BlockSpec(memory_space=pl.ANY)
    vmem_spec = pl.BlockSpec(memory_space=pltpu.VMEM)
    return pl.pallas_call(
        gru_kernel,
        out_shape=(jax.ShapeDtypeStruct((STEPS, BATCH, OWN), BF16), jax.ShapeDtypeStruct((2, BATCH, OWN), F32)),
        in_specs=[any_spec] * 7 + [vmem_spec] * 3,
        out_specs=(vmem_spec, vmem_spec),
        scratch_shapes=[
            pltpu.VMEM((2, HALF, 3 * HALF), BF16),
            pltpu.VMEM((2, 2, STEPS, BATCH, 3 * PART), F32),
            pltpu.VMEM((STEPS, BATCH, 3 * PART), F32),
            pltpu.VMEM((STEPS * BATCH, 2 * ROWS), BF16),
            pltpu.VMEM((2 * ROWS, 3 * PART), BF16),
            pltpu.VMEM((4, BATCH, ROWS), F32),
            pltpu.VMEM((STEPS + 1, 2, BATCH, HALF), BF16),
            pltpu.VMEM((2, 2, BATCH, HALF), BF16),
            pltpu.VMEM((BATCH, HALF), F32),
            pltpu.VMEM((4, STEPS, BATCH, OWN), BF16),
            pltpu.VMEM((STEPS, BATCH, OWN), BF16),
            pltpu.VMEM((4, BATCH, OWN), F32),
            pltpu.VMEM((2, BATCH, OWN), F32),
            dma((1,)), dma((2,)), dma((3,)), dma((2, 3)),
            dma((2,)), dma((4,)),
            dma((2, 3)), dma((2, 3)), dma((2, 3)),
            dma((2, 3)), dma((2, 2, 3, 2)),
            dma((2, 3)), dma((4, 3)),
            dma((CHUNKS,)), dma((STEPS, 2, 2)),
            dma((RING, 2, 2)), dma((STEPS + 1, 2)),
            dma((RING,)), dma((2,)), dma((2,)),
            dma((4, CHUNKS)), dma((CHUNKS,)),
            dma((4,)), dma((2,)),
        ],
        compiler_params=pltpu.CompilerParams(has_side_effects=True, vmem_limit_bytes=62 * 2**20),
        name="gru",
    )(*operands)


def solution(mesh):
    seq_spec = P(None, "data", "row")
    out_spec = P(None, "data", ("col", "row"))
    wide_spec = P("row", None, "col")
    square_spec = P("row", "col")
    bias_spec = P(None, "col")

    def device_body(x_rows, h_rows, wx_l1, whru_l1, whn_l1, bias_l1, wx_l2, whru_l2, whn_l2, bias_l2):
        def by_gate(weights):
            return weights.transpose(1, 0, 2)

        return gru_call(
            x_rows.reshape(STEPS * BATCH, ROWS), by_gate(wx_l1), by_gate(wx_l2), by_gate(whru_l1), by_gate(whru_l2),
            whn_l1, whn_l2, h_rows, bias_l1, bias_l2)

    return jax.shard_map(
        device_body,
        mesh=mesh,
        in_specs=(seq_spec, seq_spec, wide_spec, wide_spec, square_spec, bias_spec, wide_spec, wide_spec, square_spec, bias_spec),
        out_specs=(out_spec, out_spec),
        check_vma=False,
    )
```

```python
import functools

import jax
import jax.numpy as jnp
from jax import lax
from jax.experimental import pallas as pl
from jax.experimental.pallas import tpu as pltpu
from jax.sharding import PartitionSpec as P

MESH = pl.DeviceIdType.MESH
F32 = jnp.float32
BF16 = jnp.bfloat16

STEPS = 64
BATCH = 8
HALF = 1280
ROWS = 640
PART = 640
OWN = 320
CHUNK = 8
CHUNKS = STEPS // CHUNK
LEAD = 4
AHEAD = 12
RING = 4


def gru_kernel(x_in, wx1_in, wx2_in, ru1_in, ru2_in, n1_in, n2_in, h_in, bias1, bias2, seq_out, fin_out,
               w, pbuf, psrc, xs, wx1, h0, hid, rhb, state, outbuf, oscr, finsrc, finbuf,
               x_send, x_recv, v_send, v_recv, z_send, z_recv, s_send, s_recv, t_send,
               w_send, w_recv, wx_send, wx_recv, q_send, q_recv, b_send, b_recv, p_send, p_recv, h_send, h_recv,
               n_send, r_send, r_recv, o_send, o_recv, f_send, f_recv):
    row = lax.axis_index("row")
    col = lax.axis_index("col")
    chip = row // 2
    core = row % 2
    other = 1 - core
    hub = chip == col
    layer = chip

    def device(r, c):
        return {"row": r, "col": c}

    def remote(src, dst, send, recv, r, c):
        return pltpu.make_async_remote_copy(
            src_ref=src, dst_ref=dst, send_sem=send, recv_sem=recv,
            device_id=device(r, c), device_id_type=MESH)

    def arrived(ref, sem):
        pltpu.make_async_copy(ref, ref, sem).wait()

    def start(spec):
        src, dst, send, recv, r, c = spec
        here = (r == row) & (c == col)

        @pl.when(here)
        def _():
            pltpu.make_async_copy(src, dst, recv).start()

        @pl.when(jnp.logical_not(here))
        def _():
            remote(src, dst, send, recv, r, c).start()

    def finish(spec):
        src, dst, send, recv, r, c = spec
        here = (r == row) & (c == col)

        @pl.when(jnp.logical_not(here))
        def _():
            remote(src, dst, send, recv, r, c).wait_send()

    slot = jnp.where(hub, 0, 1)
    my_rows = pl.ds(core * ROWS, ROWS)
    my_cols = pl.ds(pl.multiple_of(core * ROWS, ROWS), ROWS)

    def gate_cols(g):
        return pl.ds(g * HALF, HALF)

    def weight(l, g):
        return (n1_in, n2_in)[l] if g == 2 else (ru1_in, ru2_in)[l].at[g]

    def x_copy(to):
        return x_in, xs.at[:, my_cols], x_send.at[0], x_recv.at[core], 2 * chip + to, col

    def wx1_copy(to, g):
        half = pl.ds(pl.multiple_of(to * PART, PART), PART)
        return (wx1_in.at[g, :, half], wx1.at[my_rows, pl.ds(g * PART, PART)], v_send.at[g], v_recv.at[core, g],
                2 * chip + to, col)

    def h0_copy(to):
        return h_in.at[col], h0.at[row], z_send.at[to], z_recv.at[row], 2 * col + to, col

    def w_copy(l, g):
        return (weight(l, g), w.at[slot, my_rows, gate_cols(g)], w_send.at[l, g], w_recv.at[slot, core, g, 0],
                2 * l + col, l)

    def stage_rows(g):
        return pl.ds(g * (ROWS // 2), ROWS // 2)

    stage_cols = pl.ds(3 * PART, HALF)

    def stage_copy(l, h, g):
        src = weight(1 - l, g).at[pl.ds(h * (ROWS // 2), ROWS // 2)]
        r, c = (2 * (1 - l) + core, l) if h == 0 else (2 * l + core, 1 - l)
        return src, w.at[l, stage_rows(g), stage_cols], s_send.at[h, g], s_recv.at[l, g], r, c

    def forward_copy(l, g):
        h = jnp.where(col == l, 0, 1)
        rows = pl.ds(core * ROWS + h * (ROWS // 2), ROWS // 2)
        return (w.at[l, stage_rows(g), stage_cols], w.at[0, rows, gate_cols(g)], t_send.at[l, g],
                w_recv.at[0, core, g, h], 2 * (1 - l) + l, 1 - l)

    def wx_copy(half, g):
        return (wx2_in.at[g, :, pl.ds(half * PART, PART)], w.at[chip, my_rows, pl.ds(g * PART, PART)],
                wx_send.at[half, g], wx_recv.at[row, g], 2 * (1 - col) + half, col)

    def q_copy():
        return psrc, pbuf.at[0, core], q_send.at[0], q_recv.at[core], 0, 0

    def b_copy(t, steps):
        at = pl.ds(t, steps)
        return psrc.at[at], pbuf.at[1, core, at], b_send.at[t % AHEAD], b_recv.at[t], core, 1

    def p_copy(t):
        return psrc.at[t], pbuf.at[chip, core, t], p_send.at[t % RING], p_recv.at[t, core], col, 0

    def send_p(t):
        @pl.when(chip == 0)
        def _():
            @pl.when(t == 0)
            def _():
                arrived(pbuf.at[1, core, pl.ds(0, LEAD)], b_recv.at[0])

            @pl.when(t == LEAD)
            def _():
                arrived(pbuf.at[1, core, pl.ds(LEAD, AHEAD - LEAD)], b_recv.at[LEAD])

            @pl.when(t >= AHEAD)
            def _():
                arrived(pbuf.at[1, core, t], b_recv.at[t])
            psrc[t] = psrc[t] + pbuf[1, core, t]
        start(p_copy(t))

    for to in (core, other):
        start(x_copy(to))
        for g in range(3):
            start(wx1_copy(to, g))
    for to in range(2):
        start(h0_copy(to))
    for l in range(2):
        @pl.when(hub & (chip == l))
        def _():
            for g in range(3):
                for h in range(2):
                    start(stage_copy(l, h, g))
            for g in range(3):
                start(w_copy(l, g))

    @pl.when(jnp.logical_not(hub))
    def _():
        for g in range(2):
            for l in range(2):
                start(w_copy(l, g))

    for b in range(2):
        arrived(xs.at[:, pl.ds(b * ROWS, ROWS)], x_recv.at[b])
        for g in range(3):
            arrived(wx1.at[pl.ds(b * ROWS, ROWS), pl.ds(g * PART, PART)], v_recv.at[b, g])

    def bias_of(ref, g):
        return ref[g:g + 1, my_cols]

    def project_x(k, carry):
        lines = xs[pl.ds(k * CHUNK * BATCH, CHUNK * BATCH), :]
        for g in range(3):
            total = jnp.dot(lines, wx1[:, g * PART:(g + 1) * PART], preferred_element_type=F32)
            total = total + jnp.where(chip == 0, bias_of(bias1, g), 0.0)
            psrc[pl.ds(k * CHUNK, CHUNK), :, g * PART:(g + 1) * PART] = total.reshape(CHUNK, BATCH, PART)
        return carry

    lax.fori_loop(0, CHUNKS, project_x, 0)

    for l in range(2):
        @pl.when(hub & (chip == l))
        def _():
            if l == 0:
                start(q_copy())
            for g in range(3):
                for h in range(2):
                    finish(stage_copy(l, h, g))
            if l == 1:
                start(b_copy(0, LEAD))
                finish(b_copy(0, LEAD))
            for g in range(3):
                for half in range(2):
                    start(wx_copy(half, g))
            if l == 1:
                for g in range(3):
                    for half in range(2):
                        finish(wx_copy(half, g))
                start(b_copy(LEAD, AHEAD - LEAD))

    @pl.when(jnp.logical_not(hub))
    def _():
        for l in range(2):
            start(w_copy(l, 2))
        for g in range(3):
            for half in range(2):
                start(wx_copy(half, g))
        for g in range(3):
            for l in range(2):
                arrived(w.at[l, stage_rows(g), stage_cols], s_recv.at[l, g])
                start(forward_copy(l, g))

        def lead(t, carry):
            send_p(t)
            return carry
        lax.fori_loop(0, LEAD, lead, 0)
        for g in range(3):
            for l in range(2):
                finish(w_copy(l, g))
                finish(forward_copy(l, g))

    @pl.when(hub)
    def _():
        first = layer == 0
        for i in range(4):
            arrived(h0.at[i], z_recv.at[i])
        for b in range(2):
            hid[0, b] = jnp.concatenate([h0[2 * b], h0[2 * b + 1]], axis=1).astype(BF16)
        state[...] = jnp.concatenate([h0[2 * core], h0[2 * core + 1]], axis=1)

        joined = first & (core == 0)

        @pl.when(joined)
        def _():
            for b in range(2):
                arrived(pbuf.at[0, b], q_recv.at[b])

        @pl.when(jnp.logical_not(joined))
        def _():
            def clear(t, carry):
                for b in range(2):
                    pbuf[1, b, t] = jnp.zeros((BATCH, 3 * PART), F32)
                return carry
            lax.fori_loop(0, STEPS, clear, 0)

        def weights_in(s, b, g, h, rows):
            at = pl.ds(b * ROWS + h * (ROWS // 2), rows)
            arrived(w.at[s, at, gate_cols(g)], w_recv.at[s, b, g, h])

        for g in range(3):
            for b in range(2):
                weights_in(1, b, g, 0, ROWS)

                @pl.when(core == chip)
                def _():
                    weights_in(0, b, g, 0, ROWS)

                @pl.when(core != chip)
                def _():
                    for h in range(2):
                        weights_in(0, b, g, h, ROWS // 2)

        def partner(t):
            return remote(hid.at[t, core], hid.at[t, core], n_send.at[t % RING], h_recv.at[t, core],
                          2 * chip + other, col)

        def helper(t, y, b):
            return remote(hid.at[t, core], hid.at[t, core], h_send.at[t % RING, y, b], h_recv.at[t, core],
                          2 * (1 - y) + b, y)

        def piece(i, k):
            at = pl.ds(k * CHUNK, CHUNK)
            return remote(outbuf.at[i, at], oscr.at[at], o_send.at[i, k], o_recv.at[k], i, core)

        def mine(i):
            return (row == i) & (col == core)

        def gate(t, g):
            cols = pl.ds(g * PART, PART)
            return jnp.concatenate(
                [pbuf[0, b, t, :, cols] + pbuf[1, b, t, :, cols] for b in range(2)], axis=1)

        def tick(t, carry):
            for b in range(2):
                arrived(pbuf.at[jnp.where(joined, 1, 0), b, t], p_recv.at[t, b])

            ru_own = jnp.dot(hid[t, core], w[0, :, 0:2 * HALF], preferred_element_type=F32)

            @pl.when(t > 0)
            def _():
                partner(t).wait_send()
                arrived(hid.at[t, other], h_recv.at[t, other])

            r_sum = ru_own[:, 0:HALF] + jnp.dot(hid[t, other], w[1, :, 0:HALF], preferred_element_type=F32)
            reset = jax.nn.sigmoid(gate(t, 0) + r_sum)
            q = t % 2
            rhb[q, core] = (reset * state[...]).astype(BF16)
            swap = remote(rhb.at[q, core], rhb.at[q, core], r_send.at[q], r_recv.at[q], 2 * chip + other, col)
            swap.start()
            u_sum = ru_own[:, HALF:] + jnp.dot(hid[t, other], w[1, :, HALF:2 * HALF], preferred_element_type=F32)
            update = jax.nn.sigmoid(gate(t, 1) + u_sum)
            n_sum = gate(t, 2) + jnp.dot(rhb[q, core], w[0, :, 2 * HALF:], preferred_element_type=F32)
            swap.wait_send()
            arrived(rhb.at[q, other], r_recv.at[q])
            n_sum = n_sum + jnp.dot(rhb[q, other], w[1, :, 2 * HALF:], preferred_element_type=F32)
            cand = jnp.tanh(n_sum)
            h_next = (1.0 - update) * cand + update * state[...]
            state[...] = h_next
            h_bf = h_next.astype(BF16)
            hid[t + 1, core] = h_bf

            @pl.when(t < STEPS - 1)
            def _():
                partner(t + 1).start()

            @pl.when(first)
            def _():
                for y in range(2):
                    for b in range(2):
                        @pl.when(t >= RING)
                        def _():
                            helper(t + 1 - RING, y, b).wait_send()
                        helper(t + 1, y, b).start()

            @pl.when(jnp.logical_not(first))
            def _():
                for i in range(4):
                    outbuf[i, t] = h_bf[:, i * OWN:(i + 1) * OWN]

                @pl.when(t + AHEAD < STEPS)
                def _():
                    @pl.when(t == 1)
                    def _():
                        finish(b_copy(LEAD, AHEAD - LEAD))

                    @pl.when(t > 0)
                    def _():
                        finish(b_copy(t - 1 + AHEAD, 1))
                    start(b_copy(t + AHEAD, 1))

                @pl.when(t % CHUNK == CHUNK - 1)
                def _():
                    for i in range(4):
                        @pl.when(jnp.logical_not(mine(i)))
                        def _():
                            piece(i, t // CHUNK).start()
            return carry

        lax.fori_loop(0, STEPS, tick, 0)

        last = state[...]
        for i in range(4):
            finsrc[i] = last[:, i * OWN:(i + 1) * OWN]

        def fin_copy(i):
            return remote(finsrc.at[i], finbuf.at[layer], f_send.at[i], f_recv.at[layer], i, core)

        for i in range(4):
            @pl.when(mine(i))
            def _():
                finbuf[layer] = finsrc[i]

                @pl.when(jnp.logical_not(first))
                def _():
                    def take(t, carry):
                        oscr[t] = outbuf[i, t]
                        return carry
                    lax.fori_loop(0, STEPS, take, 0)

            @pl.when(jnp.logical_not(mine(i)))
            def _():
                fin_copy(i).start()

        for i in range(4):
            @pl.when(jnp.logical_not(mine(i)))
            def _():
                fin_copy(i).wait_send()

                @pl.when(jnp.logical_not(first))
                def _():
                    for k in range(CHUNKS):
                        piece(i, k).wait_send()

        @pl.when(first)
        def _():
            for t in range(STEPS + 1 - RING, STEPS + 1):
                for y in range(2):
                    for b in range(2):
                        helper(t, y, b).wait_send()

    @pl.when(jnp.logical_not(hub))
    def _():
        for g in range(3):
            for i in range(4):
                arrived(w.at[i // 2, pl.ds((i % 2) * ROWS, ROWS), pl.ds(g * PART, PART)], wx_recv.at[i, g])

        def project(t):
            return remote(pbuf.at[0, core, t], pbuf.at[0, core, t], h_send.at[t % RING, 0, 0],
                          p_recv.at[t, core], 2 + col, 1)

        def tick(t, carry):
            for b in range(2):
                arrived(hid.at[t + 1, b], h_recv.at[t + 1, b])
            total = jnp.dot(hid[t + 1, 0], w[0, :, 0:3 * PART], preferred_element_type=F32)
            total = total + jnp.dot(hid[t + 1, 1], w[1, :, 0:3 * PART], preferred_element_type=F32)
            shift = jnp.concatenate([bias_of(bias2, g) for g in range(3)], axis=1)
            pbuf[0, core, t] = total + shift

            @pl.when(t >= RING)
            def _():
                project(t - RING).wait_send()
            project(t).start()

            @pl.when(t + LEAD < STEPS)
            def _():
                finish(p_copy(t))
                send_p(t + LEAD)
            return carry

        lax.fori_loop(0, STEPS, tick, 0)
        for t in range(STEPS - RING, STEPS):
            project(t).wait_send()
            finish(p_copy(t))

    for l in range(2):
        @pl.when(hub & (chip == l))
        def _():
            for g in range(3):
                finish(w_copy(l, g))
                if l == 0:
                    for half in range(2):
                        finish(wx_copy(half, g))
            if l == 0:
                finish(q_copy())
            else:
                finish(b_copy(STEPS - 1, 1))

    @pl.when(jnp.logical_not(hub))
    def _():
        for g in range(3):
            for half in range(2):
                finish(wx_copy(half, g))
    finish(x_copy(other))
    for g in range(3):
        finish(wx1_copy(other, g))
    for to in range(2):
        finish(h0_copy(to))
    for l in range(2):
        @pl.when(jnp.logical_not((row == 2 * l + col) & (col == l)))
        def _():
            arrived(finbuf.at[l], f_recv.at[l])

    @pl.when(jnp.logical_not((row == 2 + col) & (col == 1)))
    def _():
        for k in range(CHUNKS):
            at = pl.ds(k * CHUNK, CHUNK)
            arrived(oscr.at[at], o_recv.at[k])

    def emit(t, carry):
        seq_out[t] = oscr[t]
        return carry
    lax.fori_loop(0, STEPS, emit, 0)
    fin_out[...] = finbuf[...]


def gru_call(*operands):
    dma = pltpu.SemaphoreType.DMA
    any_spec = pl.BlockSpec(memory_space=pl.ANY)
    vmem_spec = pl.BlockSpec(memory_space=pltpu.VMEM)
    return pl.pallas_call(
        gru_kernel,
        out_shape=(jax.ShapeDtypeStruct((STEPS, BATCH, OWN), BF16), jax.ShapeDtypeStruct((2, BATCH, OWN), F32)),
        in_specs=[any_spec] * 7 + [vmem_spec] * 3,
        out_specs=(vmem_spec, vmem_spec),
        scratch_shapes=[
            pltpu.VMEM((2, HALF, 3 * HALF), BF16),
            pltpu.VMEM((2, 2, STEPS, BATCH, 3 * PART), F32),
            pltpu.VMEM((STEPS, BATCH, 3 * PART), F32),
            pltpu.VMEM((STEPS * BATCH, 2 * ROWS), BF16),
            pltpu.VMEM((2 * ROWS, 3 * PART), BF16),
            pltpu.VMEM((4, BATCH, ROWS), F32),
            pltpu.VMEM((STEPS + 1, 2, BATCH, HALF), BF16),
            pltpu.VMEM((2, 2, BATCH, HALF), BF16),
            pltpu.VMEM((BATCH, HALF), F32),
            pltpu.VMEM((4, STEPS, BATCH, OWN), BF16),
            pltpu.VMEM((STEPS, BATCH, OWN), BF16),
            pltpu.VMEM((4, BATCH, OWN), F32),
            pltpu.VMEM((2, BATCH, OWN), F32),
            dma((1,)), dma((2,)), dma((3,)), dma((2, 3)),
            dma((2,)), dma((4,)),
            dma((2, 3)), dma((2, 3)), dma((2, 3)),
            dma((2, 3)), dma((2, 2, 3, 2)),
            dma((2, 3)), dma((4, 3)),
            dma((1,)), dma((2,)), dma((AHEAD,)), dma((STEPS,)),
            dma((RING,)), dma((STEPS, 2)),
            dma((RING, 2, 2)), dma((STEPS + 1, 2)),
            dma((RING,)), dma((2,)), dma((2,)),
            dma((4, CHUNKS)), dma((CHUNKS,)),
            dma((4,)), dma((2,)),
        ],
        compiler_params=pltpu.CompilerParams(has_side_effects=True, vmem_limit_bytes=62 * 2**20),
        name="gru",
    )(*operands)


def solution(mesh):
    seq_spec = P(None, "data", "row")
    out_spec = P(None, "data", ("col", "row"))
    wide_spec = P("row", None, "col")
    square_spec = P("row", "col")
    bias_spec = P(None, "col")

    def device_body(x_rows, h_rows, wx_l1, whru_l1, whn_l1, bias_l1, wx_l2, whru_l2, whn_l2, bias_l2):
        def by_gate(weights):
            return weights.transpose(1, 0, 2)

        return gru_call(
            x_rows.reshape(STEPS * BATCH, ROWS), by_gate(wx_l1), by_gate(wx_l2), by_gate(whru_l1), by_gate(whru_l2),
            whn_l1, whn_l2, h_rows, bias_l1, bias_l2)

    return jax.shard_map(
        device_body,
        mesh=mesh,
        in_specs=(seq_spec, seq_spec, wide_spec, wide_spec, square_spec, bias_spec, wide_spec, wide_spec, square_spec, bias_spec),
        out_specs=(out_spec, out_spec),
        check_vma=False,
    )
```

```python
import functools

import jax
import jax.numpy as jnp
from jax import lax
from jax.experimental import pallas as pl
from jax.experimental.pallas import tpu as pltpu
from jax.sharding import PartitionSpec as P

MESH = pl.DeviceIdType.MESH
F32 = jnp.float32
BF16 = jnp.bfloat16

STEPS = 64
BATCH = 8
HALF = 1280
ROWS = 640
PART = 640
OWN = 320
CHUNK = 8
CHUNKS = STEPS // CHUNK
LEAD = 4
AHEAD = 12
RING = 4
CUT = (0, 768, HALF)


def gru_kernel(x_in, wx1_in, wx2_in, ru1_in, ru2_in, n1_in, n2_in, h_in, bias1, bias2, seq_out, fin_out,
               w, pbuf, psrc, xs, wx1, h0, hid, rhb, state, outbuf, oscr, finsrc, finbuf,
               x_send, x_recv, v_send, v_recv, z_send, z_recv, s_send, s_recv, t_send,
               w_send, w_recv, wx_send, wx_recv, q_send, q_recv, b_send, b_recv, p_send, p_recv, h_send, h_recv,
               n_send, r_send, r_recv, o_send, o_recv, f_send, f_recv):
    row = lax.axis_index("row")
    col = lax.axis_index("col")
    chip = row // 2
    core = row % 2
    other = 1 - core
    hub = chip == col
    layer = chip

    def device(r, c):
        return {"row": r, "col": c}

    def remote(src, dst, send, recv, r, c):
        return pltpu.make_async_remote_copy(
            src_ref=src, dst_ref=dst, send_sem=send, recv_sem=recv,
            device_id=device(r, c), device_id_type=MESH)

    def arrived(ref, sem):
        pltpu.make_async_copy(ref, ref, sem).wait()

    def start(spec):
        src, dst, send, recv, r, c = spec
        here = (r == row) & (c == col)

        @pl.when(here)
        def _():
            pltpu.make_async_copy(src, dst, recv).start()

        @pl.when(jnp.logical_not(here))
        def _():
            remote(src, dst, send, recv, r, c).start()

    def finish(spec):
        src, dst, send, recv, r, c = spec
        here = (r == row) & (c == col)

        @pl.when(jnp.logical_not(here))
        def _():
            remote(src, dst, send, recv, r, c).wait_send()

    slot = jnp.where(hub, 0, 1)
    my_rows = pl.ds(core * ROWS, ROWS)
    my_cols = pl.ds(pl.multiple_of(core * ROWS, ROWS), ROWS)

    def gate_cols(g):
        return pl.ds(g * HALF, HALF)

    def weight(l, g):
        return (n1_in, n2_in)[l] if g == 2 else (ru1_in, ru2_in)[l].at[g]

    def x_copy(to):
        return x_in, xs.at[:, my_cols], x_send.at[0], x_recv.at[core], 2 * chip + to, col

    def wx1_copy(to, g):
        half = pl.ds(pl.multiple_of(to * PART, PART), PART)
        return (wx1_in.at[g, :, half], wx1.at[my_rows, pl.ds(g * PART, PART)], v_send.at[g], v_recv.at[core, g],
                2 * chip + to, col)

    def h0_copy(to):
        return h_in.at[col], h0.at[row], z_send.at[to], z_recv.at[row], 2 * col + to, col

    def w_copy(l, g):
        return (weight(l, g), w.at[slot, my_rows, gate_cols(g)], w_send.at[l, g], w_recv.at[slot, core, g, 0],
                2 * l + col, l)

    def stage_rows(g):
        return pl.ds(g * (ROWS // 2), ROWS // 2)

    stage_cols = pl.ds(3 * PART, HALF)

    def stage_copy(l, h, g):
        src = weight(1 - l, g).at[pl.ds(h * (ROWS // 2), ROWS // 2)]
        r, c = (2 * (1 - l) + core, l) if h == 0 else (2 * l + core, 1 - l)
        return src, w.at[l, stage_rows(g), stage_cols], s_send.at[h, g], s_recv.at[l, g], r, c

    def forward_copy(l, g):
        h = jnp.where(col == l, 0, 1)
        rows = pl.ds(core * ROWS + h * (ROWS // 2), ROWS // 2)
        return (w.at[l, stage_rows(g), stage_cols], w.at[0, rows, gate_cols(g)], t_send.at[l, g],
                w_recv.at[0, core, g, h], 2 * (1 - l) + l, 1 - l)

    def wx_copy(half, g):
        return (wx2_in.at[g, :, pl.ds(half * PART, PART)], w.at[chip, my_rows, pl.ds(g * PART, PART)],
                wx_send.at[half, g], wx_recv.at[row, g], 2 * (1 - col) + half, col)

    def q_copy():
        return psrc, pbuf.at[0, core], q_send.at[0], q_recv.at[core], 0, 0

    def b_copy(t, steps):
        at = pl.ds(t, steps)
        return psrc.at[at], pbuf.at[1, core, at], b_send.at[t % AHEAD], b_recv.at[t], core, 1

    def p_copy(t):
        return psrc.at[t], pbuf.at[chip, core, t], p_send.at[t % RING], p_recv.at[t, core], col, 0

    def send_p(t):
        @pl.when(chip == 0)
        def _():
            @pl.when(t == 0)
            def _():
                arrived(pbuf.at[1, core, pl.ds(0, LEAD)], b_recv.at[0])

            @pl.when(t == LEAD)
            def _():
                arrived(pbuf.at[1, core, pl.ds(LEAD, AHEAD - LEAD)], b_recv.at[LEAD])

            @pl.when(t >= AHEAD)
            def _():
                arrived(pbuf.at[1, core, t], b_recv.at[t])
            psrc[t] = psrc[t] + pbuf[1, core, t]
        start(p_copy(t))

    for to in (core, other):
        start(x_copy(to))
        for g in range(3):
            start(wx1_copy(to, g))
    for to in range(2):
        start(h0_copy(to))
    for l in range(2):
        @pl.when(hub & (chip == l))
        def _():
            for g in range(3):
                for h in range(2):
                    start(stage_copy(l, h, g))
            for g in range(3):
                start(w_copy(l, g))

    @pl.when(jnp.logical_not(hub))
    def _():
        for g in range(2):
            for l in range(2):
                start(w_copy(l, g))

    for b in range(2):
        arrived(xs.at[:, pl.ds(b * ROWS, ROWS)], x_recv.at[b])
        for g in range(3):
            arrived(wx1.at[pl.ds(b * ROWS, ROWS), pl.ds(g * PART, PART)], v_recv.at[b, g])

    def bias_of(ref, g):
        return ref[g:g + 1, my_cols]

    def project_x(k, carry):
        lines = xs[pl.ds(k * CHUNK * BATCH, CHUNK * BATCH), :]
        for g in range(3):
            total = jnp.dot(lines, wx1[:, g * PART:(g + 1) * PART], preferred_element_type=F32)
            total = total + jnp.where(chip == 0, bias_of(bias1, g), 0.0)
            psrc[pl.ds(k * CHUNK, CHUNK), :, g * PART:(g + 1) * PART] = total.reshape(CHUNK, BATCH, PART)
        return carry

    lax.fori_loop(0, CHUNKS, project_x, 0)

    for l in range(2):
        @pl.when(hub & (chip == l))
        def _():
            if l == 0:
                start(q_copy())
            for g in range(3):
                for h in range(2):
                    finish(stage_copy(l, h, g))
            if l == 1:
                start(b_copy(0, LEAD))
                finish(b_copy(0, LEAD))
            for g in range(3):
                for half in range(2):
                    start(wx_copy(half, g))
            if l == 1:
                for g in range(3):
                    for half in range(2):
                        finish(wx_copy(half, g))
                start(b_copy(LEAD, AHEAD - LEAD))

    @pl.when(jnp.logical_not(hub))
    def _():
        for l in range(2):
            start(w_copy(l, 2))
        for g in range(3):
            for half in range(2):
                start(wx_copy(half, g))
        for g in range(3):
            for l in range(2):
                arrived(w.at[l, stage_rows(g), stage_cols], s_recv.at[l, g])
                start(forward_copy(l, g))

        def lead(t, carry):
            send_p(t)
            return carry
        lax.fori_loop(0, LEAD, lead, 0)
        for g in range(3):
            for l in range(2):
                finish(w_copy(l, g))
                finish(forward_copy(l, g))

    @pl.when(hub)
    def _():
        first = layer == 0
        for i in range(4):
            arrived(h0.at[i], z_recv.at[i])
        for b in range(2):
            hid[0, b] = jnp.concatenate([h0[2 * b], h0[2 * b + 1]], axis=1).astype(BF16)
        state[...] = jnp.concatenate([h0[2 * core], h0[2 * core + 1]], axis=1)

        joined = first & (core == 0)

        @pl.when(joined)
        def _():
            for b in range(2):
                arrived(pbuf.at[0, b], q_recv.at[b])

        @pl.when(jnp.logical_not(joined))
        def _():
            def clear(t, carry):
                for b in range(2):
                    pbuf[1, b, t] = jnp.zeros((BATCH, 3 * PART), F32)
                return carry
            lax.fori_loop(0, STEPS, clear, 0)

        def weights_in(s, b, g, h, rows):
            at = pl.ds(b * ROWS + h * (ROWS // 2), rows)
            arrived(w.at[s, at, gate_cols(g)], w_recv.at[s, b, g, h])

        for g in range(3):
            for b in range(2):
                weights_in(1, b, g, 0, ROWS)

                @pl.when(core == chip)
                def _():
                    weights_in(0, b, g, 0, ROWS)

                @pl.when(core != chip)
                def _():
                    for h in range(2):
                        weights_in(0, b, g, h, ROWS // 2)

        def cut(i):
            return pl.ds(CUT[i], CUT[i + 1] - CUT[i])

        def partner(t, i):
            piece = hid.at[t, core, :, cut(i)]
            return remote(piece, piece, n_send.at[t % RING, i], h_recv.at[t, core, i], 2 * chip + other, col)

        def swap(q, i):
            piece = rhb.at[q, core, :, cut(i)]
            return remote(piece, piece, r_send.at[q, i], r_recv.at[q, i], 2 * chip + other, col)

        def helper(t, y, b):
            return remote(hid.at[t, core], hid.at[t, core], h_send.at[t % RING, y, b], h_recv.at[t, core, 0],
                          2 * (1 - y) + b, y)

        def piece(i, k):
            at = pl.ds(k * CHUNK, CHUNK)
            return remote(outbuf.at[i, at], oscr.at[at], o_send.at[i, k], o_recv.at[k], i, core)

        def mine(i):
            return (row == i) & (col == core)

        def gate(t, g):
            cols = pl.ds(g * PART, PART)
            return jnp.concatenate(
                [pbuf[0, b, t, :, cols] + pbuf[1, b, t, :, cols] for b in range(2)], axis=1)

        def tick(t, carry):
            for b in range(2):
                arrived(pbuf.at[jnp.where(joined, 1, 0), b, t], p_recv.at[t, b])

            q = t % 2
            lo = [slice(CUT[i], CUT[i + 1]) for i in range(2)]

            def dot(vec, mat):
                return jnp.dot(vec, mat, preferred_element_type=F32)

            def columns(g, i):
                return slice(g * HALF + CUT[i], g * HALF + CUT[i + 1])

            def sigmoid(v):
                return 0.5 * jnp.tanh(0.5 * v) + 0.5

            p_n = gate(t, 2)
            ru_own = dot(hid[t, core], w[0, :, 0:2 * HALF])
            r_base = gate(t, 0) + ru_own[:, 0:HALF]
            u_base = gate(t, 1) + ru_own[:, HALF:]

            @pl.when(t > 0)
            def _():
                for i in range(2):
                    partner(t, i).wait_send()
                    arrived(hid.at[t, other, :, cut(i)], h_recv.at[t, other, i])

            h_other = hid[t, other]
            r_oth = [dot(h_other, w[1, :, columns(0, i)]) for i in range(2)]
            u_oth = [None, None]
            for i in range(2):
                reset = sigmoid(r_base[:, lo[i]] + r_oth[i])
                rhb[q, core, :, lo[i]] = (reset * state[:, lo[i]]).astype(BF16)
                swap(q, i).start()
                u_oth[1 - i] = dot(h_other, w[1, :, columns(1, 1 - i)])
            update = [sigmoid(u_base[:, lo[i]] + u_oth[i]) for i in range(2)]
            n_own = p_n + dot(rhb[q, core], w[0, :, 2 * HALF:])
            swap(q, 0).wait_send()
            arrived(rhb.at[q, other, :, cut(0)], r_recv.at[q, 0])
            n_own = n_own + dot(rhb[q, other, :, lo[0]], w[1, lo[0], 2 * HALF:])
            swap(q, 1).wait_send()
            arrived(rhb.at[q, other, :, cut(1)], r_recv.at[q, 1])
            n_oth = [dot(rhb[q, other, :, lo[1]], w[1, lo[1], columns(2, i)]) for i in range(2)]
            h_parts = []
            for i in range(2):
                cand = jnp.tanh(n_own[:, lo[i]] + n_oth[i])
                h_next = (1.0 - update[i]) * cand + update[i] * state[:, lo[i]]
                state[:, lo[i]] = h_next
                h_parts.append(h_next.astype(BF16))
                hid[t + 1, core, :, lo[i]] = h_parts[i]

                @pl.when(t < STEPS - 1)
                def _():
                    partner(t + 1, i).start()

            @pl.when(first)
            def _():
                for y in range(2):
                    for b in range(2):
                        @pl.when(t >= RING)
                        def _():
                            helper(t + 1 - RING, y, b).wait_send()
                        helper(t + 1, y, b).start()

            @pl.when(jnp.logical_not(first))
            def _():
                h_bf = jnp.concatenate(h_parts, axis=1)
                for i in range(4):
                    outbuf[i, t] = h_bf[:, i * OWN:(i + 1) * OWN]

                @pl.when(t + AHEAD < STEPS)
                def _():
                    @pl.when(t == 1)
                    def _():
                        finish(b_copy(LEAD, AHEAD - LEAD))

                    @pl.when(t > 0)
                    def _():
                        finish(b_copy(t - 1 + AHEAD, 1))
                    start(b_copy(t + AHEAD, 1))

                @pl.when(t % CHUNK == CHUNK - 1)
                def _():
                    for i in range(4):
                        @pl.when(jnp.logical_not(mine(i)))
                        def _():
                            piece(i, t // CHUNK).start()
            return carry

        lax.fori_loop(0, STEPS, tick, 0)

        last = state[...]
        for i in range(4):
            finsrc[i] = last[:, i * OWN:(i + 1) * OWN]

        def fin_copy(i):
            return remote(finsrc.at[i], finbuf.at[layer], f_send.at[i], f_recv.at[layer], i, core)

        for i in range(4):
            @pl.when(mine(i))
            def _():
                finbuf[layer] = finsrc[i]

                @pl.when(jnp.logical_not(first))
                def _():
                    def take(t, carry):
                        oscr[t] = outbuf[i, t]
                        return carry
                    lax.fori_loop(0, STEPS, take, 0)

            @pl.when(jnp.logical_not(mine(i)))
            def _():
                fin_copy(i).start()

        for i in range(4):
            @pl.when(jnp.logical_not(mine(i)))
            def _():
                fin_copy(i).wait_send()

                @pl.when(jnp.logical_not(first))
                def _():
                    for k in range(CHUNKS):
                        piece(i, k).wait_send()

        @pl.when(first)
        def _():
            for t in range(STEPS + 1 - RING, STEPS + 1):
                for y in range(2):
                    for b in range(2):
                        helper(t, y, b).wait_send()

    @pl.when(jnp.logical_not(hub))
    def _():
        for g in range(3):
            for i in range(4):
                arrived(w.at[i // 2, pl.ds((i % 2) * ROWS, ROWS), pl.ds(g * PART, PART)], wx_recv.at[i, g])

        def project(t):
            return remote(pbuf.at[0, core, t], pbuf.at[0, core, t], h_send.at[t % RING, 0, 0],
                          p_recv.at[t, core], 2 + col, 1)

        def tick(t, carry):
            for b in range(2):
                arrived(hid.at[t + 1, b], h_recv.at[t + 1, b, 0])
            total = jnp.dot(hid[t + 1, 0], w[0, :, 0:3 * PART], preferred_element_type=F32)
            total = total + jnp.dot(hid[t + 1, 1], w[1, :, 0:3 * PART], preferred_element_type=F32)
            shift = jnp.concatenate([bias_of(bias2, g) for g in range(3)], axis=1)
            pbuf[0, core, t] = total + shift

            @pl.when(t >= RING)
            def _():
                project(t - RING).wait_send()
            project(t).start()

            @pl.when(t + LEAD < STEPS)
            def _():
                finish(p_copy(t))
                send_p(t + LEAD)
            return carry

        lax.fori_loop(0, STEPS, tick, 0)
        for t in range(STEPS - RING, STEPS):
            project(t).wait_send()
            finish(p_copy(t))

    for l in range(2):
        @pl.when(hub & (chip == l))
        def _():
            for g in range(3):
                finish(w_copy(l, g))
                if l == 0:
                    for half in range(2):
                        finish(wx_copy(half, g))
            if l == 0:
                finish(q_copy())
            else:
                finish(b_copy(STEPS - 1, 1))

    @pl.when(jnp.logical_not(hub))
    def _():
        for g in range(3):
            for half in range(2):
                finish(wx_copy(half, g))
    finish(x_copy(other))
    for g in range(3):
        finish(wx1_copy(other, g))
    for to in range(2):
        finish(h0_copy(to))
    for l in range(2):
        @pl.when(jnp.logical_not((row == 2 * l + col) & (col == l)))
        def _():
            arrived(finbuf.at[l], f_recv.at[l])

    @pl.when(jnp.logical_not((row == 2 + col) & (col == 1)))
    def _():
        for k in range(CHUNKS):
            at = pl.ds(k * CHUNK, CHUNK)
            arrived(oscr.at[at], o_recv.at[k])

    def emit(t, carry):
        seq_out[t] = oscr[t]
        return carry
    lax.fori_loop(0, STEPS, emit, 0)
    fin_out[...] = finbuf[...]


def gru_call(*operands):
    dma = pltpu.SemaphoreType.DMA
    any_spec = pl.BlockSpec(memory_space=pl.ANY)
    vmem_spec = pl.BlockSpec(memory_space=pltpu.VMEM)
    return pl.pallas_call(
        gru_kernel,
        out_shape=(jax.ShapeDtypeStruct((STEPS, BATCH, OWN), BF16), jax.ShapeDtypeStruct((2, BATCH, OWN), F32)),
        in_specs=[any_spec] * 7 + [vmem_spec] * 3,
        out_specs=(vmem_spec, vmem_spec),
        scratch_shapes=[
            pltpu.VMEM((2, HALF, 3 * HALF), BF16),
            pltpu.VMEM((2, 2, STEPS, BATCH, 3 * PART), F32),
            pltpu.VMEM((STEPS, BATCH, 3 * PART), F32),
            pltpu.VMEM((STEPS * BATCH, 2 * ROWS), BF16),
            pltpu.VMEM((2 * ROWS, 3 * PART), BF16),
            pltpu.VMEM((4, BATCH, ROWS), F32),
            pltpu.VMEM((STEPS + 1, 2, BATCH, HALF), BF16),
            pltpu.VMEM((2, 2, BATCH, HALF), BF16),
            pltpu.VMEM((BATCH, HALF), F32),
            pltpu.VMEM((4, STEPS, BATCH, OWN), BF16),
            pltpu.VMEM((STEPS, BATCH, OWN), BF16),
            pltpu.VMEM((4, BATCH, OWN), F32),
            pltpu.VMEM((2, BATCH, OWN), F32),
            dma((1,)), dma((2,)), dma((3,)), dma((2, 3)),
            dma((2,)), dma((4,)),
            dma((2, 3)), dma((2, 3)), dma((2, 3)),
            dma((2, 3)), dma((2, 2, 3, 2)),
            dma((2, 3)), dma((4, 3)),
            dma((1,)), dma((2,)), dma((AHEAD,)), dma((STEPS,)),
            dma((RING,)), dma((STEPS, 2)),
            dma((RING, 2, 2)), dma((STEPS + 1, 2, 2)),
            dma((RING, 2)), dma((2, 2)), dma((2, 2)),
            dma((4, CHUNKS)), dma((CHUNKS,)),
            dma((4,)), dma((2,)),
        ],
        compiler_params=pltpu.CompilerParams(has_side_effects=True, vmem_limit_bytes=62 * 2**20),
        name="gru",
    )(*operands)


def solution(mesh):
    seq_spec = P(None, "data", "row")
    out_spec = P(None, "data", ("col", "row"))
    wide_spec = P("row", None, "col")
    square_spec = P("row", "col")
    bias_spec = P(None, "col")

    def device_body(x_rows, h_rows, wx_l1, whru_l1, whn_l1, bias_l1, wx_l2, whru_l2, whn_l2, bias_l2):
        def by_gate(weights):
            return weights.transpose(1, 0, 2)

        return gru_call(
            x_rows.reshape(STEPS * BATCH, ROWS), by_gate(wx_l1), by_gate(wx_l2), by_gate(whru_l1), by_gate(whru_l2),
            whn_l1, whn_l2, h_rows, bias_l1, bias_l2)

    return jax.shard_map(
        device_body,
        mesh=mesh,
        in_specs=(seq_spec, seq_spec, wide_spec, wide_spec, square_spec, bias_spec, wide_spec, wide_spec, square_spec, bias_spec),
        out_specs=(out_spec, out_spec),
        check_vma=False,
    )
```

```python
import functools

import jax
import jax.numpy as jnp
from jax import lax
from jax.experimental import pallas as pl
from jax.experimental.pallas import tpu as pltpu
from jax.sharding import PartitionSpec as P

MESH = pl.DeviceIdType.MESH
F32 = jnp.float32
BF16 = jnp.bfloat16

STEPS = 64
BATCH = 8
HALF = 1280
ROWS = 640
PART = 640
OWN = 320
CHUNK = 8
CHUNKS = STEPS // CHUNK
LEAD = 5
AHEAD = 9
RING = 4
CUT = (0, 512, HALF)


def gru_kernel(x_in, wx1_in, wx2_in, ru1_in, ru2_in, n1_in, n2_in, h_in, bias1, bias2, seq_out, fin_out,
               w, pbuf, psrc, xs, wx1, h0, hid, rhb, state, outbuf, finsrc,
               x_send, x_recv, v_send, v_recv, z_send, z_recv, s_send, s_recv, t_send,
               w_send, w_recv, wx_send, wx_recv, q_send, q_recv, b_send, b_recv, p_send, p_recv, h_send, h_recv,
               n_send, r_send, r_recv, o_send, o_recv, f_send, f_recv):
    row = lax.axis_index("row")
    col = lax.axis_index("col")
    chip = row // 2
    core = row % 2
    other = 1 - core
    hub = chip == col
    layer = chip

    def device(r, c):
        return {"row": r, "col": c}

    def remote(src, dst, send, recv, r, c):
        return pltpu.make_async_remote_copy(
            src_ref=src, dst_ref=dst, send_sem=send, recv_sem=recv,
            device_id=device(r, c), device_id_type=MESH)

    def arrived(ref, sem):
        pltpu.make_async_copy(ref, ref, sem).wait()

    def start(spec):
        src, dst, send, recv, r, c = spec
        here = (r == row) & (c == col)

        @pl.when(here)
        def _():
            pltpu.make_async_copy(src, dst, recv).start()

        @pl.when(jnp.logical_not(here))
        def _():
            remote(src, dst, send, recv, r, c).start()

    def finish(spec):
        src, dst, send, recv, r, c = spec
        here = (r == row) & (c == col)

        @pl.when(jnp.logical_not(here))
        def _():
            remote(src, dst, send, recv, r, c).wait_send()

    slot = jnp.where(hub, 0, 1)
    my_rows = pl.ds(core * ROWS, ROWS)
    my_cols = pl.ds(pl.multiple_of(core * ROWS, ROWS), ROWS)

    def gate_cols(g):
        return pl.ds(g * HALF, HALF)

    def weight(l, g):
        return (n1_in, n2_in)[l] if g == 2 else (ru1_in, ru2_in)[l].at[g]

    def x_copy(to):
        return x_in, xs.at[:, my_cols], x_send.at[0], x_recv.at[core], 2 * chip + to, col

    def wx1_copy(to, g):
        half = pl.ds(pl.multiple_of(to * PART, PART), PART)
        return (wx1_in.at[g, :, half], wx1.at[my_rows, pl.ds(g * PART, PART)], v_send.at[g], v_recv.at[core, g],
                2 * chip + to, col)

    def h0_copy(to):
        return h_in.at[col], h0.at[row], z_send.at[to], z_recv.at[row], 2 * col + to, col

    def w_copy(l, g):
        return (weight(l, g), w.at[slot, my_rows, gate_cols(g)], w_send.at[l, g], w_recv.at[slot, core, g, 0],
                2 * l + col, l)

    def stage_rows(g):
        return pl.ds(g * (ROWS // 2), ROWS // 2)

    stage_cols = pl.ds(3 * PART, HALF)

    def stage_copy(l, h, g):
        src = weight(1 - l, g).at[pl.ds(h * (ROWS // 2), ROWS // 2)]
        r, c = (2 * (1 - l) + core, l) if h == 0 else (2 * l + core, 1 - l)
        return src, w.at[l, stage_rows(g), stage_cols], s_send.at[h, g], s_recv.at[l, g], r, c

    def forward_copy(l, g):
        h = jnp.where(col == l, 0, 1)
        rows = pl.ds(core * ROWS + h * (ROWS // 2), ROWS // 2)
        return (w.at[l, stage_rows(g), stage_cols], w.at[0, rows, gate_cols(g)], t_send.at[l, g],
                w_recv.at[0, core, g, h], 2 * (1 - l) + l, 1 - l)

    def wx_copy(half, g):
        return (wx2_in.at[g, :, pl.ds(half * PART, PART)], w.at[chip, my_rows, pl.ds(g * PART, PART)],
                wx_send.at[half, g], wx_recv.at[row, g], 2 * (1 - col) + half, col)

    def q_copy():
        return psrc, pbuf.at[0, core], q_send.at[0], q_recv.at[core], 0, 0

    def b_copy(t, steps):
        at = pl.ds(t, steps)
        return psrc.at[at], pbuf.at[1, core, at], b_send.at[t % AHEAD], b_recv.at[t], core, 1

    def p_copy(t):
        return psrc.at[t], pbuf.at[chip, core, t], p_send.at[t % LEAD], p_recv.at[t, core], col, 0

    def send_p(t):
        @pl.when(chip == 0)
        def _():
            @pl.when(t == 0)
            def _():
                arrived(pbuf.at[1, core, pl.ds(0, LEAD)], b_recv.at[0])

            @pl.when(t == LEAD)
            def _():
                arrived(pbuf.at[1, core, pl.ds(LEAD, AHEAD - LEAD)], b_recv.at[LEAD])

            @pl.when(t >= AHEAD)
            def _():
                arrived(pbuf.at[1, core, t], b_recv.at[t])
            psrc[t] = psrc[t] + pbuf[1, core, t]
        start(p_copy(t))

    for to in (core, other):
        start(x_copy(to))
        for g in range(3):
            start(wx1_copy(to, g))
    for to in range(2):
        start(h0_copy(to))
    for l in range(2):
        @pl.when(hub & (chip == l))
        def _():
            for g in range(3):
                for h in range(2):
                    start(stage_copy(l, h, g))
            for g in range(3):
                start(w_copy(l, g))

    @pl.when(jnp.logical_not(hub))
    def _():
        for g in range(2):
            for l in range(2):
                start(w_copy(l, g))

    for b in range(2):
        arrived(xs.at[:, pl.ds(b * ROWS, ROWS)], x_recv.at[b])
        for g in range(3):
            arrived(wx1.at[pl.ds(b * ROWS, ROWS), pl.ds(g * PART, PART)], v_recv.at[b, g])

    def bias_of(ref, g):
        return ref[g:g + 1, my_cols]

    def project_x(k, carry):
        lines = xs[pl.ds(k * CHUNK * BATCH, CHUNK * BATCH), :]
        for g in range(3):
            total = jnp.dot(lines, wx1[:, g * PART:(g + 1) * PART], preferred_element_type=F32)
            total = total + jnp.where(chip == 0, bias_of(bias1, g), 0.0)
            psrc[pl.ds(k * CHUNK, CHUNK), :, g * PART:(g + 1) * PART] = total.reshape(CHUNK, BATCH, PART)
        return carry

    lax.fori_loop(0, CHUNKS, project_x, 0)

    for l in range(2):
        @pl.when(hub & (chip == l))
        def _():
            if l == 0:
                start(q_copy())
            for g in range(3):
                for h in range(2):
                    finish(stage_copy(l, h, g))
            if l == 1:
                start(b_copy(0, LEAD))
                finish(b_copy(0, LEAD))
            for g in range(3):
                for half in range(2):
                    start(wx_copy(half, g))
            if l == 1:
                for g in range(3):
                    for half in range(2):
                        finish(wx_copy(half, g))
                start(b_copy(LEAD, AHEAD - LEAD))

    @pl.when(jnp.logical_not(hub))
    def _():
        for l in range(2):
            start(w_copy(l, 2))
        for g in range(3):
            for half in range(2):
                start(wx_copy(half, g))
        for g in range(3):
            for l in range(2):
                arrived(w.at[l, stage_rows(g), stage_cols], s_recv.at[l, g])
                start(forward_copy(l, g))

        def lead(t, carry):
            send_p(t)
            return carry
        lax.fori_loop(0, LEAD, lead, 0)
        for g in range(3):
            for l in range(2):
                finish(w_copy(l, g))
                finish(forward_copy(l, g))

    @pl.when(hub)
    def _():
        first = layer == 0
        for i in range(4):
            arrived(h0.at[i], z_recv.at[i])
        for b in range(2):
            hid[0, b] = jnp.concatenate([h0[2 * b], h0[2 * b + 1]], axis=1).astype(BF16)
        state[...] = jnp.concatenate([h0[2 * core], h0[2 * core + 1]], axis=1)

        joined = first & (core == 0)

        @pl.when(joined)
        def _():
            for b in range(2):
                arrived(pbuf.at[0, b], q_recv.at[b])

        @pl.when(jnp.logical_not(joined))
        def _():
            def clear(t, carry):
                for b in range(2):
                    pbuf[1, b, t] = jnp.zeros((BATCH, 3 * PART), F32)
                return carry
            lax.fori_loop(0, STEPS, clear, 0)

        def weights_in(s, b, g, h, rows):
            at = pl.ds(b * ROWS + h * (ROWS // 2), rows)
            arrived(w.at[s, at, gate_cols(g)], w_recv.at[s, b, g, h])

        for g in range(3):
            for b in range(2):
                weights_in(1, b, g, 0, ROWS)

                @pl.when(core == chip)
                def _():
                    weights_in(0, b, g, 0, ROWS)

                @pl.when(core != chip)
                def _():
                    for h in range(2):
                        weights_in(0, b, g, h, ROWS // 2)

        def cut(i):
            return pl.ds(CUT[i], CUT[i + 1] - CUT[i])

        def partner(t, i):
            piece = hid.at[t, core, :, cut(i)]
            return remote(piece, piece, n_send.at[t % RING, i], h_recv.at[t, core, i], 2 * chip + other, col)

        def swap(q, i):
            piece = rhb.at[q, core, :, cut(i)]
            return remote(piece, piece, r_send.at[q, i], r_recv.at[q, i], 2 * chip + other, col)

        def helper(t, y, b):
            return remote(hid.at[t, core], hid.at[t, core], h_send.at[t % RING, y, b], h_recv.at[t, core, 0],
                          2 * (1 - y) + b, y)

        def piece(i, k):
            at = pl.ds(k * CHUNK, CHUNK)
            return outbuf.at[i, at], seq_out.at[at], o_send.at[i, k], o_recv.at[k], i, core

        def gate(t, g):
            cols = pl.ds(g * PART, PART)
            return jnp.concatenate(
                [pbuf[0, b, t, :, cols] + pbuf[1, b, t, :, cols] for b in range(2)], axis=1)

        def tick(t, carry):
            q = t % 2
            lo = [slice(CUT[i], CUT[i + 1]) for i in range(2)]

            def dot(vec, mat):
                return jnp.dot(vec, mat, preferred_element_type=F32)

            def columns(g, i):
                return slice(g * HALF + CUT[i], g * HALF + CUT[i + 1])

            def sigmoid(v):
                return 0.5 * jnp.tanh(0.5 * v) + 0.5

            ru_own = dot(hid[t, core], w[0, :, 0:2 * HALF])
            for b in range(2):
                arrived(pbuf.at[jnp.where(joined, 1, 0), b, t], p_recv.at[t, b])

            def h_in_place(i):
                @pl.when(t > 0)
                def _():
                    partner(t, i).wait_send()
                    arrived(hid.at[t, other, :, cut(i)], h_recv.at[t, other, i])

            h_in_place(0)
            r_base = ru_own[:, 0:HALF] + dot(hid[t, other, :, lo[0]], w[1, lo[0], 0:HALF])
            h_in_place(1)
            r_base = gate(t, 0) + r_base
            u_base = gate(t, 1) + ru_own[:, HALF:]
            p_n = gate(t, 2)
            h_other = hid[t, other]
            r_oth = [dot(hid[t, other, :, lo[1]], w[1, lo[1], columns(0, i)]) for i in range(2)]
            u_oth = [None, None]
            for i in range(2):
                h_half = 0.5 * state[:, lo[i]]
                gated = h_half + h_half * jnp.tanh(0.5 * (r_base[:, lo[i]] + r_oth[i]))
                rhb[q, core, :, lo[i]] = gated.astype(BF16)
                swap(q, i).start()
                u_oth[1 - i] = dot(h_other, w[1, :, columns(1, 1 - i)])
            update = [sigmoid(u_base[:, lo[i]] + u_oth[i]) for i in range(2)]
            n_own = p_n + dot(rhb[q, core], w[0, :, 2 * HALF:])
            swap(q, 0).wait_send()
            arrived(rhb.at[q, other, :, cut(0)], r_recv.at[q, 0])
            n_own = n_own + dot(rhb[q, other, :, lo[0]], w[1, lo[0], 2 * HALF:])
            swap(q, 1).wait_send()
            arrived(rhb.at[q, other, :, cut(1)], r_recv.at[q, 1])
            n_oth = [dot(rhb[q, other, :, lo[1]], w[1, lo[1], columns(2, i)]) for i in range(2)]
            h_parts = []
            for i in range(2):
                cand = jnp.tanh(n_own[:, lo[i]] + n_oth[i])
                h_next = (1.0 - update[i]) * cand + update[i] * state[:, lo[i]]
                state[:, lo[i]] = h_next
                h_parts.append(h_next.astype(BF16))
                hid[t + 1, core, :, lo[i]] = h_parts[i]

                @pl.when(t < STEPS - 1)
                def _():
                    partner(t + 1, i).start()

            @pl.when(first)
            def _():
                for y in range(2):
                    for b in range(2):
                        @pl.when(t >= RING)
                        def _():
                            helper(t + 1 - RING, y, b).wait_send()
                        helper(t + 1, y, b).start()

            @pl.when(jnp.logical_not(first))
            def _():
                h_bf = jnp.concatenate(h_parts, axis=1)
                for i in range(4):
                    outbuf[i, t] = h_bf[:, i * OWN:(i + 1) * OWN]

                @pl.when(t + AHEAD < STEPS)
                def _():
                    @pl.when(t == 1)
                    def _():
                        finish(b_copy(LEAD, AHEAD - LEAD))

                    @pl.when(t > 0)
                    def _():
                        finish(b_copy(t - 1 + AHEAD, 1))
                    start(b_copy(t + AHEAD, 1))

                @pl.when(t % CHUNK == CHUNK - 1)
                def _():
                    for i in range(4):
                        start(piece(i, t // CHUNK))
            return carry

        lax.fori_loop(0, STEPS, tick, 0)

        last = state[...]
        for i in range(4):
            finsrc[i] = last[:, i * OWN:(i + 1) * OWN]

        def fin_copy(i):
            return finsrc.at[i], fin_out.at[layer], f_send.at[i], f_recv.at[layer], i, core

        for i in range(4):
            start(fin_copy(i))
        for i in range(4):
            finish(fin_copy(i))

            @pl.when(jnp.logical_not(first))
            def _():
                for k in range(CHUNKS):
                    finish(piece(i, k))

        @pl.when(first)
        def _():
            for t in range(STEPS + 1 - RING, STEPS + 1):
                for y in range(2):
                    for b in range(2):
                        helper(t, y, b).wait_send()

    @pl.when(jnp.logical_not(hub))
    def _():
        for g in range(3):
            for i in range(4):
                arrived(w.at[i // 2, pl.ds((i % 2) * ROWS, ROWS), pl.ds(g * PART, PART)], wx_recv.at[i, g])

        def project(t):
            return remote(pbuf.at[0, core, t], pbuf.at[0, core, t], h_send.at[t % RING, 0, 0],
                          p_recv.at[t, core], 2 + col, 1)

        def tick(t, carry):
            for b in range(2):
                arrived(hid.at[t + 1, b], h_recv.at[t + 1, b, 0])
            total = jnp.dot(hid[t + 1, 0], w[0, :, 0:3 * PART], preferred_element_type=F32)
            total = total + jnp.dot(hid[t + 1, 1], w[1, :, 0:3 * PART], preferred_element_type=F32)
            shift = jnp.concatenate([bias_of(bias2, g) for g in range(3)], axis=1)
            pbuf[0, core, t] = total + shift

            @pl.when(t >= RING)
            def _():
                project(t - RING).wait_send()
            project(t).start()

            @pl.when(t + LEAD < STEPS)
            def _():
                finish(p_copy(t))
                send_p(t + LEAD)
            return carry

        lax.fori_loop(0, STEPS, tick, 0)
        for t in range(STEPS - RING, STEPS):
            project(t).wait_send()
        for t in range(STEPS - LEAD, STEPS):
            finish(p_copy(t))

    for l in range(2):
        @pl.when(hub & (chip == l))
        def _():
            for g in range(3):
                finish(w_copy(l, g))
                if l == 0:
                    for half in range(2):
                        finish(wx_copy(half, g))
            if l == 0:
                finish(q_copy())
            else:
                finish(b_copy(STEPS - 1, 1))

    @pl.when(jnp.logical_not(hub))
    def _():
        for g in range(3):
            for half in range(2):
                finish(wx_copy(half, g))
    finish(x_copy(other))
    for g in range(3):
        finish(wx1_copy(other, g))
    for to in range(2):
        finish(h0_copy(to))
    for l in range(2):
        arrived(fin_out.at[l], f_recv.at[l])
    for k in range(CHUNKS):
        arrived(seq_out.at[pl.ds(k * CHUNK, CHUNK)], o_recv.at[k])


def gru_call(*operands):
    dma = pltpu.SemaphoreType.DMA
    any_spec = pl.BlockSpec(memory_space=pl.ANY)
    vmem_spec = pl.BlockSpec(memory_space=pltpu.VMEM)
    return pl.pallas_call(
        gru_kernel,
        out_shape=(jax.ShapeDtypeStruct((STEPS, BATCH, OWN), BF16), jax.ShapeDtypeStruct((2, BATCH, OWN), F32)),
        in_specs=[any_spec] * 7 + [vmem_spec] * 3,
        out_specs=(any_spec, any_spec),
        scratch_shapes=[
            pltpu.VMEM((2, HALF, 3 * HALF), BF16),
            pltpu.VMEM((2, 2, STEPS, BATCH, 3 * PART), F32),
            pltpu.VMEM((STEPS, BATCH, 3 * PART), F32),
            pltpu.VMEM((STEPS * BATCH, 2 * ROWS), BF16),
            pltpu.VMEM((2 * ROWS, 3 * PART), BF16),
            pltpu.VMEM((4, BATCH, ROWS), F32),
            pltpu.VMEM((STEPS + 1, 2, BATCH, HALF), BF16),
            pltpu.VMEM((2, 2, BATCH, HALF), BF16),
            pltpu.VMEM((BATCH, HALF), F32),
            pltpu.VMEM((4, STEPS, BATCH, OWN), BF16),
            pltpu.VMEM((4, BATCH, OWN), F32),
            dma((1,)), dma((2,)), dma((3,)), dma((2, 3)),
            dma((2,)), dma((4,)),
            dma((2, 3)), dma((2, 3)), dma((2, 3)),
            dma((2, 3)), dma((2, 2, 3, 2)),
            dma((2, 3)), dma((4, 3)),
            dma((1,)), dma((2,)), dma((AHEAD,)), dma((STEPS,)),
            dma((LEAD,)), dma((STEPS, 2)),
            dma((RING, 2, 2)), dma((STEPS + 1, 2, 2)),
            dma((RING, 2)), dma((2, 2)), dma((2, 2)),
            dma((4, CHUNKS)), dma((CHUNKS,)),
            dma((4,)), dma((2,)),
        ],
        compiler_params=pltpu.CompilerParams(has_side_effects=True, vmem_limit_bytes=62 * 2**20),
        name="gru",
    )(*operands)


def solution(mesh):
    seq_spec = P(None, "data", "row")
    out_spec = P(None, "data", ("col", "row"))
    wide_spec = P("row", None, "col")
    square_spec = P("row", "col")
    bias_spec = P(None, "col")

    def device_body(x_rows, h_rows, wx_l1, whru_l1, whn_l1, bias_l1, wx_l2, whru_l2, whn_l2, bias_l2):
        def by_gate(weights):
            return weights.transpose(1, 0, 2)

        return gru_call(
            x_rows.reshape(STEPS * BATCH, ROWS), by_gate(wx_l1), by_gate(wx_l2), by_gate(whru_l1), by_gate(whru_l2),
            whn_l1, whn_l2, h_rows, bias_l1, bias_l2)

    return jax.shard_map(
        device_body,
        mesh=mesh,
        in_specs=(seq_spec, seq_spec, wide_spec, wide_spec, square_spec, bias_spec, wide_spec, wide_spec, square_spec, bias_spec),
        out_specs=(out_spec, out_spec),
        check_vma=False,
    )
```

```python
import functools

import jax
import jax.numpy as jnp
from jax import lax
from jax.experimental import pallas as pl
from jax.experimental.pallas import tpu as pltpu
from jax.sharding import PartitionSpec as P

MESH = pl.DeviceIdType.MESH
F32 = jnp.float32
BF16 = jnp.bfloat16

STEPS = 64
BATCH = 8
HALF = 1280
ROWS = 640
PART = 640
OWN = 320
CHUNK = 8
CHUNKS = STEPS // CHUNK
LEAD = 5
AHEAD = 8
RING = 4
EARLY = 256
CUT = (0, 512, HALF)


def gru_kernel(x_in, wx1_in, wx2_in, ru1_in, ru2_in, n1_in, n2_in, h_in, bias1, bias2, seq_out, fin_out,
               w, pbuf, psrc, xs, wx1, h0, hid, rhb, state, early, outbuf, finsrc,
               x_send, x_recv, v_send, v_recv, z_send, z_recv, s_send, s_recv, t_send,
               w_send, w_recv, wx_send, wx_recv, q_send, q_recv, b_send, b_recv, p_send, p_recv, h_send, h_recv,
               n_send, r_send, r_recv, o_send, o_recv, f_send, f_recv):
    row = lax.axis_index("row")
    col = lax.axis_index("col")
    chip = row // 2
    core = row % 2
    other = 1 - core
    hub = chip == col
    layer = chip

    def device(r, c):
        return {"row": r, "col": c}

    def remote(src, dst, send, recv, r, c):
        return pltpu.make_async_remote_copy(
            src_ref=src, dst_ref=dst, send_sem=send, recv_sem=recv,
            device_id=device(r, c), device_id_type=MESH)

    def arrived(ref, sem):
        pltpu.make_async_copy(ref, ref, sem).wait()

    def start(spec):
        src, dst, send, recv, r, c = spec
        here = (r == row) & (c == col)

        @pl.when(here)
        def _():
            pltpu.make_async_copy(src, dst, recv).start()

        @pl.when(jnp.logical_not(here))
        def _():
            remote(src, dst, send, recv, r, c).start()

    def finish(spec):
        src, dst, send, recv, r, c = spec
        here = (r == row) & (c == col)

        @pl.when(jnp.logical_not(here))
        def _():
            remote(src, dst, send, recv, r, c).wait_send()

    slot = jnp.where(hub, 0, 1)
    my_rows = pl.ds(core * ROWS, ROWS)
    my_cols = pl.ds(pl.multiple_of(core * ROWS, ROWS), ROWS)

    def gate_cols(g):
        return pl.ds(g * HALF, HALF)

    def weight(l, g):
        return (n1_in, n2_in)[l] if g == 2 else (ru1_in, ru2_in)[l].at[g]

    def x_copy(to):
        return x_in, xs.at[:, my_cols], x_send.at[0], x_recv.at[core], 2 * chip + to, col

    def wx1_copy(to, g):
        half = pl.ds(pl.multiple_of(to * PART, PART), PART)
        return (wx1_in.at[g, :, half], wx1.at[my_rows, pl.ds(g * PART, PART)], v_send.at[g], v_recv.at[core, g],
                2 * chip + to, col)

    def h0_copy(to):
        return h_in.at[col], h0.at[row], z_send.at[to], z_recv.at[row], 2 * col + to, col

    def w_copy(l, g):
        return (weight(l, g), w.at[slot, my_rows, gate_cols(g)], w_send.at[l, g], w_recv.at[slot, core, g, 0],
                2 * l + col, l)

    def stage_rows(g):
        return pl.ds(g * (ROWS // 2), ROWS // 2)

    stage_cols = pl.ds(3 * PART, HALF)

    def stage_copy(l, h, g):
        src = weight(1 - l, g).at[pl.ds(h * (ROWS // 2), ROWS // 2)]
        r, c = (2 * (1 - l) + core, l) if h == 0 else (2 * l + core, 1 - l)
        return src, w.at[l, stage_rows(g), stage_cols], s_send.at[h, g], s_recv.at[l, g], r, c

    def forward_copy(l, g):
        h = jnp.where(col == l, 0, 1)
        rows = pl.ds(core * ROWS + h * (ROWS // 2), ROWS // 2)
        return (w.at[l, stage_rows(g), stage_cols], w.at[0, rows, gate_cols(g)], t_send.at[l, g],
                w_recv.at[0, core, g, h], 2 * (1 - l) + l, 1 - l)

    def wx_copy(half, g):
        return (wx2_in.at[g, :, pl.ds(half * PART, PART)], w.at[chip, my_rows, pl.ds(g * PART, PART)],
                wx_send.at[half, g], wx_recv.at[row, g], 2 * (1 - col) + half, col)

    def q_copy():
        return psrc, pbuf.at[0, core], q_send.at[0], q_recv.at[core], 0, 0

    def b_copy(t, steps):
        at = pl.ds(t, steps)
        return psrc.at[at], pbuf.at[1, core, at], b_send.at[t % AHEAD], b_recv.at[t], core, 1

    def p_copy(t):
        return psrc.at[t], pbuf.at[chip, core, t], p_send.at[t % LEAD], p_recv.at[t, core], col, 0

    def send_p(t):
        @pl.when(chip == 0)
        def _():
            @pl.when(t == 0)
            def _():
                arrived(pbuf.at[1, core, pl.ds(0, LEAD)], b_recv.at[0])

            @pl.when(t == LEAD)
            def _():
                arrived(pbuf.at[1, core, pl.ds(LEAD, AHEAD - LEAD)], b_recv.at[LEAD])

            @pl.when(t >= AHEAD)
            def _():
                arrived(pbuf.at[1, core, t], b_recv.at[t])
            psrc[t] = psrc[t] + pbuf[1, core, t]
        start(p_copy(t))

    for to in (core, other):
        start(x_copy(to))
        for g in range(3):
            start(wx1_copy(to, g))
    for to in range(2):
        start(h0_copy(to))
    for l in range(2):
        @pl.when(hub & (chip == l))
        def _():
            for g in range(3):
                for h in range(2):
                    start(stage_copy(l, h, g))
            for g in range(3):
                start(w_copy(l, g))

    @pl.when(jnp.logical_not(hub))
    def _():
        for g in range(2):
            for l in range(2):
                start(w_copy(l, g))

    for b in range(2):
        arrived(xs.at[:, pl.ds(b * ROWS, ROWS)], x_recv.at[b])
        for g in range(3):
            arrived(wx1.at[pl.ds(b * ROWS, ROWS), pl.ds(g * PART, PART)], v_recv.at[b, g])

    def bias_of(ref, g):
        return ref[g:g + 1, my_cols]

    def project_x(k, carry):
        lines = xs[pl.ds(k * CHUNK * BATCH, CHUNK * BATCH), :]
        for g in range(3):
            total = jnp.dot(lines, wx1[:, g * PART:(g + 1) * PART], preferred_element_type=F32)
            total = total + jnp.where(chip == 0, bias_of(bias1, g), 0.0)
            psrc[pl.ds(k * CHUNK, CHUNK), :, g * PART:(g + 1) * PART] = total.reshape(CHUNK, BATCH, PART)
        return carry

    lax.fori_loop(0, CHUNKS, project_x, 0)

    for l in range(2):
        @pl.when(hub & (chip == l))
        def _():
            if l == 0:
                start(q_copy())
            for g in range(3):
                for h in range(2):
                    finish(stage_copy(l, h, g))
            if l == 1:
                start(b_copy(0, LEAD))
                finish(b_copy(0, LEAD))
            for g in range(3):
                for half in range(2):
                    start(wx_copy(half, g))
            if l == 1:
                for g in range(3):
                    for half in range(2):
                        finish(wx_copy(half, g))
                start(b_copy(LEAD, AHEAD - LEAD))

    @pl.when(jnp.logical_not(hub))
    def _():
        for l in range(2):
            start(w_copy(l, 2))
        for g in range(3):
            for half in range(2):
                start(wx_copy(half, g))
        for g in range(3):
            for l in range(2):
                arrived(w.at[l, stage_rows(g), stage_cols], s_recv.at[l, g])
                start(forward_copy(l, g))

        def lead(t, carry):
            send_p(t)
            return carry
        lax.fori_loop(0, LEAD, lead, 0)
        for g in range(3):
            for l in range(2):
                finish(w_copy(l, g))
                finish(forward_copy(l, g))

    @pl.when(hub)
    def _():
        first = layer == 0
        for i in range(4):
            arrived(h0.at[i], z_recv.at[i])
        for b in range(2):
            hid[0, b] = jnp.concatenate([h0[2 * b], h0[2 * b + 1]], axis=1).astype(BF16)
        state[...] = jnp.concatenate([h0[2 * core], h0[2 * core + 1]], axis=1)

        joined = first & (core == 0)

        @pl.when(joined)
        def _():
            for b in range(2):
                arrived(pbuf.at[0, b], q_recv.at[b])

        @pl.when(jnp.logical_not(joined))
        def _():
            def clear(t, carry):
                for b in range(2):
                    pbuf[1, b, t] = jnp.zeros((BATCH, 3 * PART), F32)
                return carry
            lax.fori_loop(0, STEPS, clear, 0)

        def weights_in(s, b, g, h, rows):
            at = pl.ds(b * ROWS + h * (ROWS // 2), rows)
            arrived(w.at[s, at, gate_cols(g)], w_recv.at[s, b, g, h])

        for g in range(3):
            for b in range(2):
                weights_in(1, b, g, 0, ROWS)

                @pl.when(core == chip)
                def _():
                    weights_in(0, b, g, 0, ROWS)

                @pl.when(core != chip)
                def _():
                    for h in range(2):
                        weights_in(0, b, g, h, ROWS // 2)

        def cut(i):
            return pl.ds(CUT[i], CUT[i + 1] - CUT[i])

        def partner(t, i):
            piece = hid.at[t, core, :, cut(i)]
            return remote(piece, piece, n_send.at[t % RING, i], h_recv.at[t, core, i], 2 * chip + other, col)

        def swap(q, i):
            piece = rhb.at[q, core, :, cut(i)]
            return remote(piece, piece, r_send.at[q, i], r_recv.at[q, i], 2 * chip + other, col)

        def helper(t, y, b):
            return remote(hid.at[t, core], hid.at[t, core], h_send.at[t % RING, y, b], h_recv.at[t, core, 0],
                          2 * (1 - y) + b, y)

        def piece(i, k):
            at = pl.ds(k * CHUNK, CHUNK)
            return outbuf.at[i, at], seq_out.at[at], o_send.at[i, k], o_recv.at[k], i, core

        def gate(t, g):
            cols = pl.ds(g * PART, PART)
            return jnp.concatenate(
                [pbuf[0, b, t, :, cols] + pbuf[1, b, t, :, cols] for b in range(2)], axis=1)

        def early_dot(t):
            return jnp.dot(hid[t, core, :, 0:EARLY], w[0, 0:EARLY, 0:2 * HALF], preferred_element_type=F32)

        early[...] = early_dot(0)

        def tick(t, carry):
            q = t % 2
            lo = [slice(CUT[i], CUT[i + 1]) for i in range(2)]

            def dot(vec, mat):
                return jnp.dot(vec, mat, preferred_element_type=F32)

            def columns(g, i):
                return slice(g * HALF + CUT[i], g * HALF + CUT[i + 1])

            def sigmoid(v):
                return 0.5 * jnp.tanh(0.5 * v) + 0.5

            ru_own = early[...] + dot(hid[t, core, :, EARLY:], w[0, EARLY:, 0:2 * HALF])
            for b in range(2):
                arrived(pbuf.at[jnp.where(joined, 1, 0), b, t], p_recv.at[t, b])

            @pl.when(first & (t > 0))
            def _():
                for y in range(2):
                    for b in range(2):
                        @pl.when(t > RING)
                        def _():
                            helper(t - RING, y, b).wait_send()
                        helper(t, y, b).start()

            def h_in_place(i):
                @pl.when(t > 0)
                def _():
                    partner(t, i).wait_send()
                    arrived(hid.at[t, other, :, cut(i)], h_recv.at[t, other, i])

            h_in_place(0)
            r_base = ru_own[:, 0:HALF] + dot(hid[t, other, :, lo[0]], w[1, lo[0], 0:HALF])
            h_in_place(1)
            r_base = gate(t, 0) + r_base
            u_base = gate(t, 1) + ru_own[:, HALF:]
            p_n = gate(t, 2)
            h_other = hid[t, other]
            r_oth = [dot(hid[t, other, :, lo[1]], w[1, lo[1], columns(0, i)]) for i in range(2)]
            u_oth = [None, None]
            for i in range(2):
                h_half = 0.5 * state[:, lo[i]]
                gated = h_half + h_half * jnp.tanh(0.5 * (r_base[:, lo[i]] + r_oth[i]))
                rhb[q, core, :, lo[i]] = gated.astype(BF16)
                swap(q, i).start()
                u_oth[1 - i] = dot(h_other, w[1, :, columns(1, 1 - i)])
            update = [sigmoid(u_base[:, lo[i]] + u_oth[i]) for i in range(2)]
            n_own = p_n + dot(rhb[q, core], w[0, :, 2 * HALF:])
            swap(q, 0).wait_send()
            arrived(rhb.at[q, other, :, cut(0)], r_recv.at[q, 0])
            n_own = n_own + dot(rhb[q, other, :, lo[0]], w[1, lo[0], 2 * HALF:])
            swap(q, 1).wait_send()
            arrived(rhb.at[q, other, :, cut(1)], r_recv.at[q, 1])
            n_oth = [dot(rhb[q, other, :, lo[1]], w[1, lo[1], columns(2, i)]) for i in range(2)]
            h_parts = []
            for i in range(2):
                cand = jnp.tanh(n_own[:, lo[i]] + n_oth[i])
                h_next = (1.0 - update[i]) * cand + update[i] * state[:, lo[i]]
                state[:, lo[i]] = h_next
                h_parts.append(h_next.astype(BF16))
                hid[t + 1, core, :, lo[i]] = h_parts[i]

                @pl.when(t < STEPS - 1)
                def _():
                    partner(t + 1, i).start()

                if i == 0:
                    early[...] = early_dot(t + 1)

            @pl.when(jnp.logical_not(first))
            def _():
                h_bf = jnp.concatenate(h_parts, axis=1)
                for i in range(4):
                    outbuf[i, t] = h_bf[:, i * OWN:(i + 1) * OWN]

                @pl.when(t + AHEAD < STEPS)
                def _():
                    @pl.when(t == 1)
                    def _():
                        finish(b_copy(LEAD, AHEAD - LEAD))

                    @pl.when(t > 0)
                    def _():
                        finish(b_copy(t - 1 + AHEAD, 1))
                    start(b_copy(t + AHEAD, 1))

                @pl.when(t % CHUNK == CHUNK - 1)
                def _():
                    for i in range(4):
                        start(piece(i, t // CHUNK))
            return carry

        lax.fori_loop(0, STEPS, tick, 0)

        last = state[...]
        for i in range(4):
            finsrc[i] = last[:, i * OWN:(i + 1) * OWN]

        def fin_copy(i):
            return finsrc.at[i], fin_out.at[layer], f_send.at[i], f_recv.at[layer], i, core

        for i in range(4):
            start(fin_copy(i))
        for i in range(4):
            finish(fin_copy(i))

            @pl.when(jnp.logical_not(first))
            def _():
                for k in range(CHUNKS):
                    finish(piece(i, k))

        @pl.when(first)
        def _():
            for y in range(2):
                for b in range(2):
                    helper(STEPS - RING, y, b).wait_send()
                    helper(STEPS, y, b).start()
            for t in range(STEPS + 1 - RING, STEPS + 1):
                for y in range(2):
                    for b in range(2):
                        helper(t, y, b).wait_send()

    @pl.when(jnp.logical_not(hub))
    def _():
        for g in range(3):
            for i in range(4):
                arrived(w.at[i // 2, pl.ds((i % 2) * ROWS, ROWS), pl.ds(g * PART, PART)], wx_recv.at[i, g])

        def project(t):
            return remote(pbuf.at[0, core, t], pbuf.at[0, core, t], h_send.at[t % RING, 0, 0],
                          p_recv.at[t, core], 2 + col, 1)

        def tick(t, carry):
            for b in range(2):
                arrived(hid.at[t + 1, b], h_recv.at[t + 1, b, 0])
            total = jnp.dot(hid[t + 1, 0], w[0, :, 0:3 * PART], preferred_element_type=F32)
            total = total + jnp.dot(hid[t + 1, 1], w[1, :, 0:3 * PART], preferred_element_type=F32)
            shift = jnp.concatenate([bias_of(bias2, g) for g in range(3)], axis=1)
            pbuf[0, core, t] = total + shift

            @pl.when(t >= RING)
            def _():
                project(t - RING).wait_send()
            project(t).start()

            @pl.when(t + LEAD < STEPS)
            def _():
                finish(p_copy(t))
                send_p(t + LEAD)
            return carry

        lax.fori_loop(0, STEPS, tick, 0)
        for t in range(STEPS - RING, STEPS):
            project(t).wait_send()
        for t in range(STEPS - LEAD, STEPS):
            finish(p_copy(t))

    for l in range(2):
        @pl.when(hub & (chip == l))
        def _():
            for g in range(3):
                finish(w_copy(l, g))
                if l == 0:
                    for half in range(2):
                        finish(wx_copy(half, g))
            if l == 0:
                finish(q_copy())
            else:
                finish(b_copy(STEPS - 1, 1))

    @pl.when(jnp.logical_not(hub))
    def _():
        for g in range(3):
            for half in range(2):
                finish(wx_copy(half, g))
    finish(x_copy(other))
    for g in range(3):
        finish(wx1_copy(other, g))
    for to in range(2):
        finish(h0_copy(to))
    for l in range(2):
        arrived(fin_out.at[l], f_recv.at[l])
    for k in range(CHUNKS):
        arrived(seq_out.at[pl.ds(k * CHUNK, CHUNK)], o_recv.at[k])


def gru_call(*operands):
    dma = pltpu.SemaphoreType.DMA
    any_spec = pl.BlockSpec(memory_space=pl.ANY)
    vmem_spec = pl.BlockSpec(memory_space=pltpu.VMEM)
    return pl.pallas_call(
        gru_kernel,
        out_shape=(jax.ShapeDtypeStruct((STEPS, BATCH, OWN), BF16), jax.ShapeDtypeStruct((2, BATCH, OWN), F32)),
        in_specs=[any_spec] * 7 + [vmem_spec] * 3,
        out_specs=(any_spec, any_spec),
        scratch_shapes=[
            pltpu.VMEM((2, HALF, 3 * HALF), BF16),
            pltpu.VMEM((2, 2, STEPS, BATCH, 3 * PART), F32),
            pltpu.VMEM((STEPS, BATCH, 3 * PART), F32),
            pltpu.VMEM((STEPS * BATCH, 2 * ROWS), BF16),
            pltpu.VMEM((2 * ROWS, 3 * PART), BF16),
            pltpu.VMEM((4, BATCH, ROWS), F32),
            pltpu.VMEM((STEPS + 1, 2, BATCH, HALF), BF16),
            pltpu.VMEM((2, 2, BATCH, HALF), BF16),
            pltpu.VMEM((BATCH, HALF), F32),
            pltpu.VMEM((BATCH, 2 * HALF), F32),
            pltpu.VMEM((4, STEPS, BATCH, OWN), BF16),
            pltpu.VMEM((4, BATCH, OWN), F32),
            dma((1,)), dma((2,)), dma((3,)), dma((2, 3)),
            dma((2,)), dma((4,)),
            dma((2, 3)), dma((2, 3)), dma((2, 3)),
            dma((2, 3)), dma((2, 2, 3, 2)),
            dma((2, 3)), dma((4, 3)),
            dma((1,)), dma((2,)), dma((AHEAD,)), dma((STEPS,)),
            dma((LEAD,)), dma((STEPS, 2)),
            dma((RING, 2, 2)), dma((STEPS + 1, 2, 2)),
            dma((RING, 2)), dma((2, 2)), dma((2, 2)),
            dma((4, CHUNKS)), dma((CHUNKS,)),
            dma((4,)), dma((2,)),
        ],
        compiler_params=pltpu.CompilerParams(has_side_effects=True, vmem_limit_bytes=62 * 2**20),
        name="gru",
    )(*operands)


def solution(mesh):
    seq_spec = P(None, "data", "row")
    out_spec = P(None, "data", ("col", "row"))
    wide_spec = P("row", None, "col")
    square_spec = P("row", "col")
    bias_spec = P(None, "col")

    def device_body(x_rows, h_rows, wx_l1, whru_l1, whn_l1, bias_l1, wx_l2, whru_l2, whn_l2, bias_l2):
        def by_gate(weights):
            return weights.transpose(1, 0, 2)

        return gru_call(
            x_rows.reshape(STEPS * BATCH, ROWS), by_gate(wx_l1), by_gate(wx_l2), by_gate(whru_l1), by_gate(whru_l2),
            whn_l1, whn_l2, h_rows, bias_l1, bias_l2)

    return jax.shard_map(
        device_body,
        mesh=mesh,
        in_specs=(seq_spec, seq_spec, wide_spec, wide_spec, square_spec, bias_spec, wide_spec, wide_spec, square_spec, bias_spec),
        out_specs=(out_spec, out_spec),
        check_vma=False,
    )
```

```python
import functools

import jax
import jax.numpy as jnp
from jax import lax
from jax.experimental import pallas as pl
from jax.experimental.pallas import tpu as pltpu
from jax.sharding import PartitionSpec as P

MESH = pl.DeviceIdType.MESH
F32 = jnp.float32
BF16 = jnp.bfloat16

STEPS = 64
BATCH = 8
HALF = 1280
ROWS = 640
PART = 640
OWN = 320
CHUNK = 8
CHUNKS = STEPS // CHUNK
LEAD = 5
AHEAD = 8
RING = 4
EARLY = 256
CUT = (0, 512, HALF)


def gru_kernel(x_in, wx1_in, wx2_in, ru1_in, ru2_in, n1_in, n2_in, h_in, bias1, bias2, seq_out, fin_out,
               w, pbuf, psrc, xs, wx1, h0, hid, rhb, state, early, outbuf, finsrc,
               x_send, x_recv, v_send, v_recv, z_send, z_recv, s_send, s_recv, t_send,
               w_send, w_recv, wx_send, wx_recv, q_send, q_recv, b_send, b_recv, p_send, p_recv, h_send, h_recv,
               n_send, r_send, r_recv, o_send, o_recv, f_send, f_recv):
    row = lax.axis_index("row")
    col = lax.axis_index("col")
    chip = row // 2
    core = row % 2
    other = 1 - core
    hub = chip == col
    layer = chip

    def device(r, c):
        return {"row": r, "col": c}

    def remote(src, dst, send, recv, r, c):
        return pltpu.make_async_remote_copy(
            src_ref=src, dst_ref=dst, send_sem=send, recv_sem=recv,
            device_id=device(r, c), device_id_type=MESH)

    def arrived(ref, sem):
        pltpu.make_async_copy(ref, ref, sem).wait()

    def start(spec):
        src, dst, send, recv, r, c = spec
        here = (r == row) & (c == col)

        @pl.when(here)
        def _():
            pltpu.make_async_copy(src, dst, recv).start()

        @pl.when(jnp.logical_not(here))
        def _():
            remote(src, dst, send, recv, r, c).start()

    def finish(spec):
        src, dst, send, recv, r, c = spec
        here = (r == row) & (c == col)

        @pl.when(jnp.logical_not(here))
        def _():
            remote(src, dst, send, recv, r, c).wait_send()

    slot = jnp.where(hub, 0, 1)
    my_rows = pl.ds(core * ROWS, ROWS)
    my_cols = pl.ds(pl.multiple_of(core * ROWS, ROWS), ROWS)

    def gate_cols(g):
        return pl.ds(g * HALF, HALF)

    def weight(l, g):
        return (n1_in, n2_in)[l] if g == 2 else (ru1_in, ru2_in)[l].at[g]

    def x_copy(to):
        return x_in, xs.at[:, my_cols], x_send.at[0], x_recv.at[core], 2 * chip + to, col

    def wx1_copy(to, g):
        half = pl.ds(pl.multiple_of(to * PART, PART), PART)
        return (wx1_in.at[g, :, half], wx1.at[my_rows, pl.ds(g * PART, PART)], v_send.at[g], v_recv.at[core, g],
                2 * chip + to, col)

    def h0_copy(to):
        return h_in.at[col], h0.at[row], z_send.at[to], z_recv.at[row], 2 * col + to, col

    def w_copy(l, g):
        return (weight(l, g), w.at[slot, my_rows, gate_cols(g)], w_send.at[l, g], w_recv.at[slot, core, g, 0],
                2 * l + col, l)

    def stage_rows(g):
        return pl.ds(g * (ROWS // 2), ROWS // 2)

    stage_cols = pl.ds(3 * PART, HALF)

    def stage_copy(l, h, g):
        src = weight(1 - l, g).at[pl.ds(h * (ROWS // 2), ROWS // 2)]
        r, c = (2 * (1 - l) + core, l) if h == 0 else (2 * l + core, 1 - l)
        return src, w.at[l, stage_rows(g), stage_cols], s_send.at[h, g], s_recv.at[l, g], r, c

    def forward_copy(l, g):
        h = jnp.where(col == l, 0, 1)
        rows = pl.ds(core * ROWS + h * (ROWS // 2), ROWS // 2)
        return (w.at[l, stage_rows(g), stage_cols], w.at[0, rows, gate_cols(g)], t_send.at[l, g],
                w_recv.at[0, core, g, h], 2 * (1 - l) + l, 1 - l)

    def wx_copy(half, g):
        return (wx2_in.at[g, :, pl.ds(half * PART, PART)], w.at[chip, my_rows, pl.ds(g * PART, PART)],
                wx_send.at[half, g], wx_recv.at[row, g], 2 * (1 - col) + half, col)

    def q_copy():
        return psrc, pbuf.at[0, core], q_send.at[0], q_recv.at[core], 0, 0

    def b_copy(t, steps):
        at = pl.ds(t, steps)
        return psrc.at[at], pbuf.at[1, core, at], b_send.at[t % AHEAD], b_recv.at[t], core, 1

    def p_copy(t):
        return psrc.at[t], pbuf.at[chip, core, t], p_send.at[t % LEAD], p_recv.at[t, core], col, 0

    def send_p(t):
        @pl.when(chip == 0)
        def _():
            @pl.when(t == 0)
            def _():
                arrived(pbuf.at[1, core, pl.ds(0, LEAD)], b_recv.at[0])

            @pl.when(t == LEAD)
            def _():
                arrived(pbuf.at[1, core, pl.ds(LEAD, AHEAD - LEAD)], b_recv.at[LEAD])

            @pl.when(t >= AHEAD)
            def _():
                arrived(pbuf.at[1, core, t], b_recv.at[t])
            psrc[t] = psrc[t] + pbuf[1, core, t]
        start(p_copy(t))

    for to in (core, other):
        start(x_copy(to))
        for g in range(3):
            start(wx1_copy(to, g))
    for to in range(2):
        start(h0_copy(to))
    for l in range(2):
        @pl.when(hub & (chip == l))
        def _():
            for g in range(3):
                for h in range(2):
                    start(stage_copy(l, h, g))
            for g in range(3):
                start(w_copy(l, g))

    @pl.when(jnp.logical_not(hub))
    def _():
        for g in range(2):
            for l in range(2):
                start(w_copy(l, g))

    for b in range(2):
        arrived(xs.at[:, pl.ds(b * ROWS, ROWS)], x_recv.at[b])
        for g in range(3):
            arrived(wx1.at[pl.ds(b * ROWS, ROWS), pl.ds(g * PART, PART)], v_recv.at[b, g])

    def bias_of(ref, g):
        return ref[g:g + 1, my_cols]

    def project_x(k, carry):
        lines = xs[pl.ds(k * CHUNK * BATCH, CHUNK * BATCH), :]
        for g in range(3):
            total = jnp.dot(lines, wx1[:, g * PART:(g + 1) * PART], preferred_element_type=F32)
            total = total + jnp.where(chip == 0, bias_of(bias1, g), 0.0)
            psrc[pl.ds(k * CHUNK, CHUNK), :, g * PART:(g + 1) * PART] = total.reshape(CHUNK, BATCH, PART)
        return carry

    lax.fori_loop(0, CHUNKS, project_x, 0)

    for l in range(2):
        @pl.when(hub & (chip == l))
        def _():
            if l == 0:
                start(q_copy())
            for g in range(3):
                for h in range(2):
                    finish(stage_copy(l, h, g))
            if l == 1:
                start(b_copy(0, LEAD))
                finish(b_copy(0, LEAD))
            for g in range(3):
                for half in range(2):
                    start(wx_copy(half, g))
            if l == 1:
                for g in range(3):
                    for half in range(2):
                        finish(wx_copy(half, g))
                start(b_copy(LEAD, AHEAD - LEAD))

    @pl.when(jnp.logical_not(hub))
    def _():
        for l in range(2):
            start(w_copy(l, 2))
        for g in range(3):
            for half in range(2):
                start(wx_copy(half, g))
        for g in range(3):
            for l in range(2):
                arrived(w.at[l, stage_rows(g), stage_cols], s_recv.at[l, g])
                start(forward_copy(l, g))
            if g == 1:
                send_p(jnp.int32(0))

        def lead(t, carry):
            send_p(t)
            return carry
        lax.fori_loop(1, LEAD, lead, 0)
        for g in range(3):
            for l in range(2):
                finish(w_copy(l, g))
                finish(forward_copy(l, g))

    @pl.when(hub)
    def _():
        first = layer == 0
        for i in range(4):
            arrived(h0.at[i], z_recv.at[i])
        for b in range(2):
            hid[0, b] = jnp.concatenate([h0[2 * b], h0[2 * b + 1]], axis=1).astype(BF16)
        state[...] = jnp.concatenate([h0[2 * core], h0[2 * core + 1]], axis=1)

        joined = first & (core == 0)

        @pl.when(joined)
        def _():
            for b in range(2):
                arrived(pbuf.at[0, b], q_recv.at[b])

        @pl.when(jnp.logical_not(joined))
        def _():
            def clear(t, carry):
                for b in range(2):
                    pbuf[1, b, t] = jnp.zeros((BATCH, 3 * PART), F32)
                return carry
            lax.fori_loop(0, STEPS, clear, 0)

        def weights_in(s, b, g, h, rows):
            at = pl.ds(b * ROWS + h * (ROWS // 2), rows)
            arrived(w.at[s, at, gate_cols(g)], w_recv.at[s, b, g, h])

        def gate_in(g):
            for b in range(2):
                weights_in(1, b, g, 0, ROWS)

                @pl.when(core == chip)
                def _():
                    weights_in(0, b, g, 0, ROWS)

                @pl.when(core != chip)
                def _():
                    for h in range(2):
                        weights_in(0, b, g, h, ROWS // 2)

        gate_in(0)
        gate_in(1)

        def cut(i):
            return pl.ds(CUT[i], CUT[i + 1] - CUT[i])

        def partner(t, i):
            piece = hid.at[t, core, :, cut(i)]
            return remote(piece, piece, n_send.at[t % RING, i], h_recv.at[t, core, i], 2 * chip + other, col)

        def swap(q, i):
            piece = rhb.at[q, core, :, cut(i)]
            return remote(piece, piece, r_send.at[q, i], r_recv.at[q, i], 2 * chip + other, col)

        def helper(t, y, b):
            return remote(hid.at[t, core], hid.at[t, core], h_send.at[t % RING, y, b], h_recv.at[t, core, 0],
                          2 * (1 - y) + b, y)

        def piece(i, k):
            at = pl.ds(k * CHUNK, CHUNK)
            return outbuf.at[i, at], seq_out.at[at], o_send.at[i, k], o_recv.at[k], i, core

        def gate(t, g):
            cols = pl.ds(g * PART, PART)
            return jnp.concatenate(
                [pbuf[0, b, t, :, cols] + pbuf[1, b, t, :, cols] for b in range(2)], axis=1)

        def early_dot(t):
            return jnp.dot(hid[t, core, :, 0:EARLY], w[0, 0:EARLY, 0:2 * HALF], preferred_element_type=F32)

        early[...] = early_dot(0)

        def tick(t, head):
            q = t % 2
            lo = [slice(CUT[i], CUT[i + 1]) for i in range(2)]

            def dot(vec, mat):
                return jnp.dot(vec, mat, preferred_element_type=F32)

            def columns(g, i):
                return slice(g * HALF + CUT[i], g * HALF + CUT[i + 1])

            def sigmoid(v):
                return 0.5 * jnp.tanh(0.5 * v) + 0.5

            ru_own = early[...] + dot(hid[t, core, :, EARLY:], w[0, EARLY:, 0:2 * HALF])
            for b in range(2):
                arrived(pbuf.at[jnp.where(joined, 1, 0), b, t], p_recv.at[t, b])

            if not head:
              @pl.when(first)
              def _():
                for y in range(2):
                    for b in range(2):
                        @pl.when(t > RING)
                        def _():
                            helper(t - RING, y, b).wait_send()
                        helper(t, y, b).start()

            def h_in_place(i):
                if not head:
                    partner(t, i).wait_send()
                    arrived(hid.at[t, other, :, cut(i)], h_recv.at[t, other, i])

            h_in_place(0)
            r_base = ru_own[:, 0:HALF] + dot(hid[t, other, :, lo[0]], w[1, lo[0], 0:HALF])
            h_in_place(1)
            r_base = gate(t, 0) + r_base
            u_base = gate(t, 1) + ru_own[:, HALF:]
            p_n = gate(t, 2)
            h_other = hid[t, other]
            r_oth = [dot(hid[t, other, :, lo[1]], w[1, lo[1], columns(0, i)]) for i in range(2)]
            u_oth = [None, None]
            for i in range(2):
                h_half = 0.5 * state[:, lo[i]]
                gated = h_half + h_half * jnp.tanh(0.5 * (r_base[:, lo[i]] + r_oth[i]))
                rhb[q, core, :, lo[i]] = gated.astype(BF16)
                swap(q, i).start()
                u_oth[1 - i] = dot(h_other, w[1, :, columns(1, 1 - i)])
            update = [sigmoid(u_base[:, lo[i]] + u_oth[i]) for i in range(2)]
            if head:
                gate_in(2)
            n_own = p_n + dot(rhb[q, core], w[0, :, 2 * HALF:])
            swap(q, 0).wait_send()
            arrived(rhb.at[q, other, :, cut(0)], r_recv.at[q, 0])
            n_own = n_own + dot(rhb[q, other, :, lo[0]], w[1, lo[0], 2 * HALF:])
            swap(q, 1).wait_send()
            arrived(rhb.at[q, other, :, cut(1)], r_recv.at[q, 1])
            n_oth = [dot(rhb[q, other, :, lo[1]], w[1, lo[1], columns(2, i)]) for i in range(2)]
            h_parts = []
            for i in range(2):
                cand = jnp.tanh(n_own[:, lo[i]] + n_oth[i])
                h_next = (1.0 - update[i]) * cand + update[i] * state[:, lo[i]]
                state[:, lo[i]] = h_next
                h_parts.append(h_next.astype(BF16))
                hid[t + 1, core, :, lo[i]] = h_parts[i]

                @pl.when(t < STEPS - 1)
                def _():
                    partner(t + 1, i).start()

                if i == 0:
                    early[...] = early_dot(t + 1)

            @pl.when(jnp.logical_not(first))
            def _():
                h_bf = jnp.concatenate(h_parts, axis=1)
                for i in range(4):
                    outbuf[i, t] = h_bf[:, i * OWN:(i + 1) * OWN]

                @pl.when(t + AHEAD < STEPS)
                def _():
                    @pl.when(t == 1)
                    def _():
                        finish(b_copy(LEAD, AHEAD - LEAD))

                    @pl.when(t > 0)
                    def _():
                        finish(b_copy(t - 1 + AHEAD, 1))
                    start(b_copy(t + AHEAD, 1))

                @pl.when(t % CHUNK == CHUNK - 1)
                def _():
                    for i in range(4):
                        start(piece(i, t // CHUNK))

        def later(t, carry):
            tick(t, False)
            return carry

        tick(jnp.int32(0), True)
        lax.fori_loop(1, STEPS, later, 0)

        last = state[...]
        for i in range(4):
            finsrc[i] = last[:, i * OWN:(i + 1) * OWN]

        def fin_copy(i):
            return finsrc.at[i], fin_out.at[layer], f_send.at[i], f_recv.at[layer], i, core

        for i in range(4):
            start(fin_copy(i))
        for i in range(4):
            finish(fin_copy(i))

            @pl.when(jnp.logical_not(first))
            def _():
                for k in range(CHUNKS):
                    finish(piece(i, k))

        @pl.when(first)
        def _():
            for y in range(2):
                for b in range(2):
                    helper(STEPS - RING, y, b).wait_send()
                    helper(STEPS, y, b).start()
            for t in range(STEPS + 1 - RING, STEPS + 1):
                for y in range(2):
                    for b in range(2):
                        helper(t, y, b).wait_send()

    @pl.when(jnp.logical_not(hub))
    def _():
        for g in range(3):
            for i in range(4):
                arrived(w.at[i // 2, pl.ds((i % 2) * ROWS, ROWS), pl.ds(g * PART, PART)], wx_recv.at[i, g])

        def project(t):
            return remote(pbuf.at[0, core, t], pbuf.at[0, core, t], h_send.at[t % RING, 0, 0],
                          p_recv.at[t, core], 2 + col, 1)

        def tick(t, carry):
            for b in range(2):
                arrived(hid.at[t + 1, b], h_recv.at[t + 1, b, 0])
            total = jnp.dot(hid[t + 1, 0], w[0, :, 0:3 * PART], preferred_element_type=F32)
            total = total + jnp.dot(hid[t + 1, 1], w[1, :, 0:3 * PART], preferred_element_type=F32)
            shift = jnp.concatenate([bias_of(bias2, g) for g in range(3)], axis=1)
            pbuf[0, core, t] = total + shift

            @pl.when(t >= RING)
            def _():
                project(t - RING).wait_send()
            project(t).start()

            @pl.when(t + LEAD < STEPS)
            def _():
                finish(p_copy(t))
                send_p(t + LEAD)
            return carry

        lax.fori_loop(0, STEPS, tick, 0)
        for t in range(STEPS - RING, STEPS):
            project(t).wait_send()
        for t in range(STEPS - LEAD, STEPS):
            finish(p_copy(t))

    for l in range(2):
        @pl.when(hub & (chip == l))
        def _():
            for g in range(3):
                finish(w_copy(l, g))
                if l == 0:
                    for half in range(2):
                        finish(wx_copy(half, g))
            if l == 0:
                finish(q_copy())
            else:
                finish(b_copy(STEPS - 1, 1))

    @pl.when(jnp.logical_not(hub))
    def _():
        for g in range(3):
            for half in range(2):
                finish(wx_copy(half, g))
    finish(x_copy(other))
    for g in range(3):
        finish(wx1_copy(other, g))
    for to in range(2):
        finish(h0_copy(to))
    for l in range(2):
        arrived(fin_out.at[l], f_recv.at[l])
    for k in range(CHUNKS):
        arrived(seq_out.at[pl.ds(k * CHUNK, CHUNK)], o_recv.at[k])


def gru_call(*operands):
    dma = pltpu.SemaphoreType.DMA
    any_spec = pl.BlockSpec(memory_space=pl.ANY)
    vmem_spec = pl.BlockSpec(memory_space=pltpu.VMEM)
    return pl.pallas_call(
        gru_kernel,
        out_shape=(jax.ShapeDtypeStruct((STEPS, BATCH, OWN), BF16), jax.ShapeDtypeStruct((2, BATCH, OWN), F32)),
        in_specs=[any_spec] * 7 + [vmem_spec] * 3,
        out_specs=(any_spec, any_spec),
        scratch_shapes=[
            pltpu.VMEM((2, HALF, 3 * HALF), BF16),
            pltpu.VMEM((2, 2, STEPS, BATCH, 3 * PART), F32),
            pltpu.VMEM((STEPS, BATCH, 3 * PART), F32),
            pltpu.VMEM((STEPS * BATCH, 2 * ROWS), BF16),
            pltpu.VMEM((2 * ROWS, 3 * PART), BF16),
            pltpu.VMEM((4, BATCH, ROWS), F32),
            pltpu.VMEM((STEPS + 1, 2, BATCH, HALF), BF16),
            pltpu.VMEM((2, 2, BATCH, HALF), BF16),
            pltpu.VMEM((BATCH, HALF), F32),
            pltpu.VMEM((BATCH, 2 * HALF), F32),
            pltpu.VMEM((4, STEPS, BATCH, OWN), BF16),
            pltpu.VMEM((4, BATCH, OWN), F32),
            dma((1,)), dma((2,)), dma((3,)), dma((2, 3)),
            dma((2,)), dma((4,)),
            dma((2, 3)), dma((2, 3)), dma((2, 3)),
            dma((2, 3)), dma((2, 2, 3, 2)),
            dma((2, 3)), dma((4, 3)),
            dma((1,)), dma((2,)), dma((AHEAD,)), dma((STEPS,)),
            dma((LEAD,)), dma((STEPS, 2)),
            dma((RING, 2, 2)), dma((STEPS + 1, 2, 2)),
            dma((RING, 2)), dma((2, 2)), dma((2, 2)),
            dma((4, CHUNKS)), dma((CHUNKS,)),
            dma((4,)), dma((2,)),
        ],
        compiler_params=pltpu.CompilerParams(has_side_effects=True, vmem_limit_bytes=62 * 2**20),
        name="gru",
    )(*operands)


def solution(mesh):
    seq_spec = P(None, "data", "row")
    out_spec = P(None, "data", ("col", "row"))
    wide_spec = P("row", None, "col")
    square_spec = P("row", "col")
    bias_spec = P(None, "col")

    def device_body(x_rows, h_rows, wx_l1, whru_l1, whn_l1, bias_l1, wx_l2, whru_l2, whn_l2, bias_l2):
        def by_gate(weights):
            return weights.transpose(1, 0, 2)

        return gru_call(
            x_rows.reshape(STEPS * BATCH, ROWS), by_gate(wx_l1), by_gate(wx_l2), by_gate(whru_l1), by_gate(whru_l2),
            whn_l1, whn_l2, h_rows, bias_l1, bias_l2)

    return jax.shard_map(
        device_body,
        mesh=mesh,
        in_specs=(seq_spec, seq_spec, wide_spec, wide_spec, square_spec, bias_spec, wide_spec, wide_spec, square_spec, bias_spec),
        out_specs=(out_spec, out_spec),
        check_vma=False,
    )
```
